32 devices in a mesh: mem: 4 (over z), state: 8 (over y, x, core).
Axes of the slice: x: 2, y: 2, z: 4, core: 2. Of those that a mesh axis runs over, the one named last changes fastest.
Arguments:
- anomalies: bfloat16 [64, 32, 32768], P('mem', None, 'state'), may hold values from -0.75 to 0.75
- alpha: bfloat16 [64, 32, 2048], P('mem', None, 'state'), may hold values from -6 to 6
- basis: bfloat16 [2048, 32768], P(None, 'state'), may hold values from -0.1875 to 0.1875
- gradient: bfloat16 [32, 32768], P(None, 'state'), may hold values from -6 to 6
- vertical_root: float32 [32, 32], replicated, may hold values from -1 to 1
- band_gain: float32 [16], replicated, may hold values from 0.25 to 2
- band: int32 [2048], P('state'), may hold values from 0 to 15
- order: int32 [64], replicated, may hold values from 0 to 63, each once
Outputs:
- increment: float32 [32, 32768], P(None, 'state')
- alpha_grad: float32 [64, 32, 2048], P('mem', None, 'state')
The draws below stay inside these ranges and needn't reach their ends.
Inputs may be any that keep to these rules, and one draw needn't show every extreme that they name: `order`: a permutation: every member is named by exactly one slot.
All inputs are finite; a program needn't handle non-finite values.
Results may differ from the reference program's by a relative error of at most 0.0029.
Values may be sent and summed in bfloat16 or wider, within the bound.
A program may use at most 128 MiB of HBM per device.

```python
import math
import jax
import jax.numpy as jnp
from jax import lax

LEVELS = 32
MODES = 2048
BANDS = 16
MEMBERS = 64
COLUMNS = 32768


def set_ends(result, key, least, top_value):
    spot = [jax.random.randint(jax.random.fold_in(key, axis), (), 0, length) for axis, length in enumerate(result.shape)]
    main_axis = result.shape.index(max(result.shape))
    neighbour = spot[:main_axis] + [(spot[main_axis] + 1) % result.shape[main_axis]] + spot[main_axis + 1:]
    return result.at[tuple(spot)].set(least).at[tuple(neighbour)].set(top_value)


def raised(values, key, source, target, blocks, factor):
    owner, partner = [(jnp.arange(values.shape[dim]) // (values.shape[dim] // blocks)).reshape([-1 if axis == dim else 1 for axis in range(values.ndim)]) for dim in (source, target)]
    chosen = jax.random.permutation(key, blocks)[partner]
    strong = (owner == chosen) | (owner == (partner + blocks // 2) % blocks)
    return jnp.where(strong, factor * values, values)


def steps_of(own_key, extent, shards, low, top_value):
    gain, own = 1.0, jax.random.fold_in(own_key, 6)
    for axis_at, parts in shards:
        heights = jnp.exp(jax.random.uniform(jax.random.fold_in(own, axis_at), (parts,), jnp.float32, low / len(shards), top_value / len(shards)))
        gain = gain * jnp.repeat(heights, extent[axis_at] // parts).reshape([-1 if axis == axis_at else 1 for axis in range(len(extent))])
    return gain


def normal_values(own_key, shape, spread, reach, cuts=(), kind=jnp.bfloat16):
    result = jax.random.normal(own_key, shape, jnp.float32) * spread
    if len(cuts) > 0:
        result = steps_of(own_key, shape, cuts, -0.22, 0.18) * result
    return jnp.clip(result, min=-reach, max=reach).astype(kind)


def noise_with(rng, dims, scale, most, pieces, heavy, kind=jnp.bfloat16):
    array = scale * jax.random.normal(rng, dims, jnp.float32)
    if pieces:
        array = array * steps_of(rng, dims, pieces, -0.22, 0.18)
    return jnp.clip(raised(array, jax.random.fold_in(rng, 3), *heavy), -most, most).astype(kind)


def setup_inputs(seed: int = 0) -> dict:
    arg_keys = jax.random.split(jax.random.key(seed), 9)
    return {
        "anomalies": normal_values(arg_keys[0], (MEMBERS, LEVELS, COLUMNS), 0.125, 0.75, ((0, 4), (2, 8))),
        "alpha": normal_values(arg_keys[1], (MEMBERS, LEVELS, MODES), 1.0, 6.0, ((0, 4), (2, 8))),
        "basis": noise_with(arg_keys[2], (MODES, COLUMNS), MODES ** -0.5, 0.1875, ((1, 8),), (1, 0, 8, 2.0)),
        "gradient": normal_values(arg_keys[3], (LEVELS, COLUMNS), 1.0, 6.0, ((1, 8),)),
        "vertical_root": normal_values(arg_keys[4], (LEVELS, LEVELS), LEVELS ** -0.5, 1.0, (), jnp.float32),
        "band_gain": jnp.clip(jnp.exp(jax.random.uniform(arg_keys[5], (BANDS,), jnp.float32, math.log(0.25), math.log(2.0))), 0.25, 2.0),
        "band": set_ends(jax.random.randint(arg_keys[6], (MODES,), 0, BANDS), jax.random.fold_in(arg_keys[6], 1), 0, BANDS - 1).astype(jnp.int32),
        "order": jax.random.permutation(arg_keys[7], MEMBERS).astype(jnp.int32),
    }


def reference(anomalies, alpha, basis, gradient, vertical_root, band_gain, band, order):
    high = lax.Precision.HIGHEST
    onehot = (band[:, None] == jnp.arange(BANDS, dtype=jnp.int32)[None, :]).astype(jnp.float32)
    filter_gain = jnp.sum(onehot * band_gain[None, :], axis=1)
    coef = jnp.einsum("ab,jbk->jak", vertical_root, alpha.astype(jnp.float32), precision=high)
    coef = (coef * filter_gain[None, None, :]).astype(jnp.bfloat16)
    inverse = jnp.zeros((MEMBERS,), jnp.int32).at[order].set(jnp.arange(MEMBERS, dtype=jnp.int32))
    member_coef = coef[inverse]
    grad_float = gradient.astype(jnp.float32)

    def one_member(running, member_items):
        member_anom, member_c = member_items
        member_field = jnp.dot(member_c, basis, preferred_element_type=jnp.float32)
        running = running + member_anom.astype(jnp.float32) * member_field
        weighted = (member_anom.astype(jnp.float32) * grad_float).astype(jnp.bfloat16)
        projected = lax.dot_general(weighted, basis, (((1,), (1,)), ((), ())), preferred_element_type=jnp.float32)
        return running, projected

    increment, projected = lax.scan(one_member, jnp.zeros((LEVELS, COLUMNS), jnp.float32), (anomalies, member_coef))
    slot_proj = projected[order]
    alpha_grad = jnp.einsum("ab,jak->jbk", vertical_root, slot_proj, precision=high) * filter_gain[None, None, :]
    return increment, alpha_grad
```

```python
import functools
import types
import jax
import jax.numpy as jnp
from jax import lax
from jax.experimental import pallas as pl
from jax.experimental.pallas import tpu as pltpu
from jax.sharding import PartitionSpec as P

MESH = pl.DeviceIdType.MESH
F32 = jnp.float32
BF16 = jnp.bfloat16
NT = (((1,), (1,)), ((), ()))
LANES = 128
GROUP = 256
HALVES = 2
STRIPS = 4


def flip(a, k, n):
    out, bit = 0, 1
    while bit < n:
        out = out + lax.rem(lax.div(a, bit) + (k // bit) % 2, 2) * bit
        bit *= 2
    return out


def split(v):
    high = v.astype(BF16)
    return high, (v - high.astype(F32)).astype(BF16)


def kernel(
    zn, sn, names,
    order, band_gain, vroot_h, alpha_h, band_h, gradient_h, anomalies, basis,
    inc_out, grad_out, *scratch,
):
    r = types.SimpleNamespace(**dict(zip(names, scratch)))
    coef_held = [ref for name, ref in zip(names, scratch) if name.startswith("coef_held")]
    grad_held = [ref for name, ref in zip(names, scratch) if name.startswith("grad_held")]
    z = lax.axis_index("mem")
    s = lax.axis_index("state")
    chip, core = lax.div(s, 2), lax.rem(s, 2)
    qn = sn // 2
    partner = chip * 2 + (1 - core)
    members, levels, columns = r.anom.shape
    modes = r.alpha.shape[1]
    parts = len(coef_held)
    _, lv, gw = coef_held[0].shape
    groups = modes // gw
    rows = members * levels
    slots = zn * members
    width = columns // STRIPS
    line, square = zn == 4, qn == 4

    zpeer = [flip(z, k, zn) for k in range(zn)]
    qpeer = [flip(chip, k, qn) for k in range(qn)]
    if square:
        first = qpeer[1] * (1 - core) + qpeer[2] * core
        second = qpeer[2] * (1 - core) + qpeer[1] * core
        chips = [qpeer[3], first, second, chip]
        chips_there = [qpeer[3], second, first, chip]
    else:
        chips = [qpeer[k] for k in range(qn - 1, -1, -1)]
        chips_there = chips

    barrier = pltpu.get_barrier_semaphore()
    for k in range(1, zn):
        pl.semaphore_signal(barrier, inc=1, device_id={"mem": zpeer[k]}, device_id_type=MESH)
    for k in range(1, qn):
        pl.semaphore_signal(barrier, inc=1, device_id={"state": qpeer[k] * 2 + core}, device_id_type=MESH)
    pl.semaphore_signal(barrier, inc=1, device_id={"state": partner}, device_id_type=MESH)

    small = [
        pltpu.make_async_copy(src, dst, r.load_sem.at[i])
        for i, (src, dst) in enumerate(
            [(vroot_h, r.vroot), (alpha_h, r.alpha), (band_h, r.band), (gradient_h, r.gradient), (anomalies, r.anom)]
        )
    ]
    for copy in small:
        copy.start()

    def load_of(g, t, n):
        here = pl.ds(g * gw, gw)
        return pltpu.make_async_copy(basis.at[t, here], r.base.at[t, here], r.base_sem.at[n])

    loads = []
    for g in range(groups):
        for i in range(qn):
            n = 2 * (g * qn + i)
            loads.append((load_of(g, chips_there[i] * 2 + 1 - core, n), load_of(g, chips[i] * 2 + core, n + 1)))
            loads[-1][0].start()
            loads[-1][1].start()

    def to(src, dst, send, recv, **where):
        return pltpu.make_async_remote_copy(
            src_ref=src, dst_ref=dst, send_sem=send, recv_sem=recv, device_id=where, device_id_type=MESH
        )

    spot = lax.broadcasted_iota(jnp.int32, r.inv_v.shape, 1)
    inverse = jnp.zeros(r.inv_v.shape, jnp.int32)
    for j in range(slots):
        inverse = jnp.where(spot == order[j], j, inverse)
    r.inv_v[...] = inverse
    inv_copy = pltpu.make_async_copy(r.inv_v, r.inv_s, r.inv_sem)
    inv_copy.start()

    own_rows = pl.ds(z * members, members)
    outer = lax.div(lax.rem(z + 1, zn), 2) == 0
    inner = jnp.logical_not(outer)
    near = 1 + lax.div(z, 2)
    mid = 3 - near
    other = 3 - z
    rim = (z - 1) * 3
    distant = 3 - rim

    class Exchange:
        def __init__(self, find, held, pack, mine, height, send, recv):
            self.find, self.held, self.pack, self.mine, self.height = find, held, pack, mine, height
            own = held.at[own_rows]
            if not line:
                self.out = [to(own, own, send.at[k], recv.at[z], mem=zpeer[k]) for k in range(1, zn)]
                self.come = [self.arrival(zpeer[k], send, recv, zpeer[k]) for k in range(1, zn)]
                return
            self.to_mid = to(own, own, send.at[0], recv.at[z], mem=mid)
            self.to_near = to(own, own, send.at[1], recv.at[z], mem=near)
            self.to_other = to(own, own, send.at[0], recv.at[z], mem=other)
            self.give = to(pack, mine, send.at[2], recv.at[z], mem=rim)
            self.given = to(pack, mine, send.at[2], recv.at[near], mem=near)
            self.come = [self.arrival(a, send, recv, other) for a in (rim, other, distant)]

        def arrival(self, a, send, recv, where):
            there = self.held.at[pl.ds(a * members, members)]
            return to(there, there, send.at[0], recv.at[a], mem=where)

        def start(self):
            if not line:
                for copy in self.out:
                    copy.start()
                return

            @pl.when(outer)
            def _():
                self.to_mid.start()
                self.to_near.start()

            @pl.when(inner)
            def _():
                self.to_other.start()

        def choose(self, out, who):
            for m in range(members):
                out[m * self.height : (m + 1) * self.height, :] = self.held[self.find(who * members + m)]

        def take_inner(self):
            for copy in self.come:
                copy.wait_recv()
            self.choose(self.pack, rim)
            self.give.start()
            self.choose(self.mine, z)

        def take_outer(self):
            self.given.wait_recv()

        def take(self):
            for copy in self.come:
                copy.wait_recv()
            self.choose(self.mine, z)

        def drain(self):
            if not line:
                for copy in self.out:
                    copy.wait_send()
                return

            @pl.when(outer)
            def _():
                self.to_mid.wait_send()
                self.to_near.wait_send()

            @pl.when(inner)
            def _():
                self.to_other.wait_send()
                self.give.wait_send()

    grid = (GROUP, levels)
    row_of = lax.broadcasted_iota(jnp.int32, grid, 0)
    level_of = lax.broadcasted_iota(jnp.int32, grid, 1)
    chunk = GROUP // HALVES
    piece_level = lax.div(row_of, chunk) * lv + lax.rem(row_of, lv)
    plain = jnp.where(lax.rem(row_of, levels) == level_of, 1.0, 0.0).astype(BF16)
    pieced = jnp.where(piece_level == level_of, 1.0, 0.0).astype(BF16)
    wide = (GROUP, GROUP)
    here_of = lax.broadcasted_iota(jnp.int32, wide, 0)
    there_of = lax.div(lax.broadcasted_iota(jnp.int32, wide, 1), levels)
    same_plain = lax.div(here_of, levels) == there_of
    same_pieced = lax.div(lax.rem(here_of, chunk), lv) == there_of

    def dot(a, b):
        return jnp.dot(a, b, preferred_element_type=F32)

    def dot_nt(a, b):
        return lax.dot_general(a, b, NT, preferred_element_type=F32)

    def blocks(tall, same):
        full = dot_nt(tall.astype(BF16), plain)
        return jnp.where(same, full, 0.0).astype(BF16)

    with jax.named_scope("coef"):
        small[0].wait()
        root_terms = split(r.vroot[...])
        root = [blocks(dot(pieced, v), same_pieced) for v in root_terms]
        root_t = [blocks(dot_nt(plain, v), same_plain) for v in root_terms]
        for v, keep in zip(root_t, (0, 1)):
            r.root_t[keep] = v
        small[1].wait()
        small[2].wait()
        band = r.band[...].reshape(1, modes)
        gain = jnp.zeros((1, modes), F32)
        for b in range(band_gain.shape[0]):
            gain = jnp.where(band == b, band_gain[b], gain)
        r.gain[...] = gain
        for n in range(rows // GROUP):
            control = r.alpha[n * GROUP : (n + 1) * GROUP, :]
            coef = (dot(root[0], control) + dot(root[1], control)) * gain
            coef = coef.astype(BF16)
            count = GROUP // levels
            for c in range(HALVES):
                for g in range(groups):
                    block = coef[c * chunk : (c + 1) * chunk, g * gw : (g + 1) * gw]
                    at = pl.ds(z * members + n * count, count)
                    coef_held[c * groups + g][at] = block.reshape(count, lv, gw)
    with jax.named_scope("barrier"):
        pl.semaphore_wait(barrier, zn - 1 + qn)

    coef_ex = [
        Exchange(
            lambda m: r.inv_s[0, m], coef_held[p], r.coef_pack.at[p], r.pick.at[p, s], lv,
            r.z_send.at[p], r.z_recv.at[p],
        )
        for p in range(parts)
    ]
    for ex in coef_ex:
        ex.start()
    grad_ex = [
        Exchange(
            lambda m: order[m], grad_held[g], r.grad_pack.at[g], r.got.at[g], levels,
            r.g_send.at[g], r.g_recv.at[g],
        )
        for g in range(groups)
    ]

    with jax.named_scope("weigh"):
        small[3].wait()
        small[4].wait()

        def weigh(m, carry):
            at = pl.ds(pl.multiple_of(m * levels, levels), levels)
            r.weighted[at, :] = (r.anom[m].astype(F32) * r.gradient[...].astype(F32)).astype(BF16)
            return carry

        lax.fori_loop(0, members, weigh, 0)

    def block_of(p, t):
        return r.pick.at[p, t]

    def share(p, t, i, where):
        return to(block_of(p, t), block_of(p, t), r.pk_send.at[p, i], r.pk_recv.at[p, t], state=where)

    class Gather:
        def __init__(self, p):
            self.p = p
            if square:
                self.out = [
                    share(p, s, 0, first * 2 + core), share(p, s, 1, second * 2 + core), share(p, s, 2, partner)
                ]
                tf, ts, td = first * 2 + core, second * 2 + core, qpeer[3] * 2 + core
                self.relay = share(p, tf, 3, second * 2 + core)
                self.arrive = [share(p, t, 4, partner) for t in (tf, ts, td)]
                self.over = [share(p, t, 4 + i, partner) for i, t in enumerate((tf, ts, td))]
            else:
                self.out = [share(p, s, k - 1, qpeer[k] * 2 + core) for k in range(1, qn)]
                self.out.append(share(p, s, qn - 1, partner))
                blocks_there = [qpeer[k] * 2 + core for k in range(1, qn)]
                self.arrive = [share(p, t, qn, partner) for t in blocks_there]
                self.over = [share(p, t, qn + i, partner) for i, t in enumerate(blocks_there)]
            self.rest = [share(p, qpeer[k] * 2 + 1 - core, 0, partner) for k in range(qn)]

        def start(self):
            for copy in self.out:
                copy.start()

        def pass_on(self):
            if square:
                self.arrive[0].wait_recv()
                self.relay.start()
                self.over[0].start()
                self.arrive[1].wait_recv()
                self.over[1].start()
            else:
                for come, go in zip(self.arrive, self.over):
                    come.wait_recv()
                    go.start()

        def pass_last(self):
            if square:
                self.arrive[2].wait_recv()
                self.over[2].start()

        def finish(self):
            for copy in self.rest:
                copy.wait_recv()

        def drain(self):
            for copy in self.out + self.over + ([self.relay] if square else []):
                copy.wait_send()

    gathers = [Gather(p) for p in range(parts)]

    def serve_inner(p):
        if line and p < parts:

            @pl.when(inner)
            def _():
                coef_ex[p].take_inner()
                gathers[p].start()

    def serve_outer(p):
        if line and p < parts:

            @pl.when(outer)
            def _():
                coef_ex[p].take_outer()
                gathers[p].start()

    def serve_all(p):
        if not line and p < parts:
            coef_ex[p].take()
            gathers[p].start()

    pairs = [
        to(r.pair_out.at[n], r.pair_in.at[n], r.pair_send.at[n], r.pair_recv.at[n], state=partner)
        for n in range(groups * qn)
    ]
    scatters = []
    for g in range(groups):
        if square:
            via = [(r.relay_in.at[g], first), (r.rs_in.at[g, 0], first), (r.rs_in.at[g, 1], second)]
        else:
            via = [(r.rs_in.at[g, i], chips[i]) for i in range(qn - 1)]
        scatters.append([
            to(r.rs_out.at[g, i], dst, r.rs_send.at[g, i], r.rs_recv.at[g, i], state=where * 2 + core)
            for i, (dst, where) in enumerate(via)
        ])

    def unit(g, i):
        n = g * qn + i
        for copy in loads[n]:
            copy.wait()
        cut = slice(g * gw, (g + 1) * gw)
        rhs = jnp.concatenate(
            [r.base[chips_there[i] * 2 + 1 - core, cut, :], r.base[chips[i] * 2 + core, cut, :]], axis=0
        )
        both = dot_nt(r.weighted[...], rhs)
        r.pair_out[n] = both[:, :gw]
        r.mine[n] = both[:, gw:]

    def combine(g, i):
        n = g * qn + i
        pairs[n].wait_recv()
        total = r.mine[n] + r.pair_in[n]
        if i == qn - 1:
            r.mine[n] = total
            return
        if square and i == 2:
            scatters[g][0].wait_recv()
            total = total + r.relay_in[g].astype(F32)
        r.rs_out[g, i] = total.astype(BF16)
        scatters[g][i].start()

    def adjoint(g):
        for copy in scatters[g][1:] if square else scatters[g]:
            copy.wait_recv()
        total = r.mine[g * qn + qn - 1]
        for i in range(r.rs_in.shape[1]):
            total = total + r.rs_in[g, i].astype(F32)
        stack = jnp.concatenate([total[n * GROUP : (n + 1) * GROUP] for n in range(rows // GROUP)], axis=1)
        high, low = split(stack)
        grad = dot(r.root_t[0], high) + dot(r.root_t[0], low) + dot(r.root_t[1], high)
        scale = r.gain[:, g * gw : (g + 1) * gw]
        count = GROUP // levels
        for n in range(rows // GROUP):
            block = (grad[:, n * gw : (n + 1) * gw] * scale).astype(BF16)
            grad_held[g][pl.ds(z * members + n * count, count)] = block.reshape(count, levels, gw)
        grad_ex[g].start()

    inv_copy.wait()
    steps = [(g, i) for g in range(groups) for i in range(qn)]
    for n, (g, i) in enumerate(steps):
        with jax.named_scope(f"unit{n}"):
            unit(g, i)
        pairs[n].start()
        if n > 0:
            combine(*steps[n - 1])
        with jax.named_scope(f"serve{n}"):
            if n == 3:
                serve_inner(0)
            if n == 5:
                serve_inner(1)
            if n == 6:
                serve_outer(0)
    with jax.named_scope("combine"):
        combine(*steps[-1])
    with jax.named_scope("serve_a"):
        serve_all(0)
        serve_all(1)
    with jax.named_scope("adjoint0"):
        adjoint(0)
    with jax.named_scope("serve_b"):
        serve_inner(2)
        serve_outer(1)
    with jax.named_scope("pass0"):
        gathers[0].pass_on()
    if groups > 1:
        with jax.named_scope("adjoint1"):
            adjoint(1)
    with jax.named_scope("serve_c"):
        serve_inner(3)
        serve_outer(2)
    with jax.named_scope("pass0l"):
        gathers[0].pass_last()
    with jax.named_scope("pass1"):
        gathers[1].pass_on()

    if line:
        def stage_of(c, j):
            return to(r.inc_out.at[c, j], r.inc_in.at[c, j], r.is_send.at[c, j], r.is_recv.at[c, j], mem=near)

        def cross_of(c, j):
            return to(r.inc_sum.at[c, j], r.inc_got.at[c, j], r.ic_send.at[c, j], r.ic_recv.at[c, j], mem=other)

        def final_of(c, j, where):
            return to(r.inc_all.at[c, j], r.inc_all.at[c, j], r.if_send.at[c, j], r.if_recv.at[c, j], mem=where)

    def spread(c, g):
        p = c * groups + g

        def part(j, carry):
            at = pl.ds(pl.multiple_of(j * width, width), width)
            cut = slice(g * gw, (g + 1) * gw)
            lhs = jnp.concatenate([r.pick[p, t] for t in range(sn)], axis=1)
            rhs = jnp.concatenate([r.base[t, cut, at] for t in range(sn)], axis=0)
            field = dot(lhs, rhs)
            if g > 0:
                field = field + r.acc[:, at]
            if g < groups - 1:
                r.acc[:, at] = field
                return carry
            run = jnp.zeros((lv, width), F32)
            for m in range(members):
                run = run + field[m * lv : (m + 1) * lv] * r.anom[m, c * lv : (c + 1) * lv, at].astype(F32)
            r.inc_part[c * lv : (c + 1) * lv, at] = run
            if line:

                @pl.when(outer)
                def _():
                    r.inc_out[c, j] = run.astype(BF16)
                    stage_of(c, j).start()

            return carry

        lax.fori_loop(0, STRIPS, part, 0)

    def each(fn):
        def step(j, carry):
            fn(j)
            return carry

        lax.fori_loop(0, STRIPS, step, 0)

    def inner_sum(c):
        def one(j):
            at = pl.ds(pl.multiple_of(j * width, width), width)
            stage_of(c, j).wait_recv()
            total = r.inc_part[c * lv : (c + 1) * lv, at] + r.inc_in[c, j].astype(F32)
            r.inc_sum[c, j] = total.astype(BF16)
            cross_of(c, j).start()

        if line:
            @pl.when(inner)
            def _():
                each(one)

    def inner_final(c):
        def one(j):
            cross_of(c, j).wait_recv()
            total = r.inc_sum[c, j].astype(F32) + r.inc_got[c, j].astype(F32)
            r.inc_all[c, j] = total.astype(BF16)
            final_of(c, j, rim).start()

        if line:
            @pl.when(inner)
            def _():
                each(one)

    def grad_inner(g):
        if line and g < groups:

            @pl.when(inner)
            def _():
                grad_ex[g].take_inner()

    with jax.named_scope("fin0"):
        gathers[0].finish()
    with jax.named_scope("spread0"):
        spread(0, 0)
    with jax.named_scope("serve_d"):
        serve_outer(3)
    if groups > 1:
        with jax.named_scope("pass1l"):
            gathers[1].pass_last()
            gathers[1].finish()
        with jax.named_scope("spread1"):
            spread(0, 1)
        with jax.named_scope("grad0"):
            grad_inner(0)
        with jax.named_scope("pass2"):
            gathers[2].pass_on()
            gathers[2].pass_last()
            gathers[2].finish()
        with jax.named_scope("spread2"):
            spread(1, 0)
        with jax.named_scope("sum0"):
            inner_sum(0)
        with jax.named_scope("pass3"):
            gathers[3].pass_on()
        with jax.named_scope("grad1"):
            grad_inner(1)
        with jax.named_scope("pass3l"):
            gathers[3].pass_last()
            gathers[3].finish()
        with jax.named_scope("spread3"):
            spread(1, 1)
    else:
        gathers[1].pass_last()
        gathers[1].finish()
        spread(1, 0)
        grad_inner(0)
        inner_sum(0)
    with jax.named_scope("final0"):
        inner_final(0)
    with jax.named_scope("sum1"):
        inner_sum(1)
    with jax.named_scope("final1"):
        inner_final(1)

    with jax.named_scope("settle"):
        if line:
            @pl.when(outer)
            def _():
                for ex in grad_ex:
                    ex.take_outer()
        else:
            for ex in grad_ex:
                ex.take()
        for g in range(groups):
            grad_out[:, g * gw : (g + 1) * gw] = r.got[g]

    if line:
        with jax.named_scope("last"):
            @pl.when(outer)
            def _():
                for c in range(HALVES):
                    each(lambda j, c=c: final_of(c, j, near).wait_recv())

            for c in range(HALVES):
                for j in range(STRIPS):
                    inc_out[c * lv : (c + 1) * lv, j * width : (j + 1) * width] = r.inc_all[c, j]

        @pl.when(outer)
        def _():
            for c in range(HALVES):
                each(lambda j, c=c: stage_of(c, j).wait_send())

        @pl.when(inner)
        def _():
            for c in range(HALVES):
                each(lambda j, c=c: cross_of(c, j).wait_send())
                each(lambda j, c=c: final_of(c, j, rim).wait_send())
    else:
        strip = columns // zn
        sums = [
            to(r.inc_out.at[k], r.inc_in.at[k], r.is_send.at[k], r.is_recv.at[k], mem=zpeer[k]) for k in range(1, zn)
        ]
        for k in range(1, zn):
            at = pl.ds(pl.multiple_of(zpeer[k] * strip, strip), strip)
            r.inc_out[k] = r.inc_part[:, at].astype(BF16)
            sums[k - 1].start()
        run = r.inc_part[:, pl.ds(pl.multiple_of(z * strip, strip), strip)]
        for k in range(1, zn):
            sums[k - 1].wait_recv()
            run = run + r.inc_in[k].astype(F32)
        r.inc_all[z] = run.astype(BF16)

        def held(k, a):
            return to(r.inc_all.at[a], r.inc_all.at[a], r.if_send.at[k], r.if_recv.at[a], mem=zpeer[k])

        shares = [held(k, z) for k in range(1, zn)]
        for copy in shares:
            copy.start()
        for k in range(1, zn):
            held(k, zpeer[k]).wait_recv()
        for b in range(zn):
            inc_out[:, b * strip : (b + 1) * strip] = r.inc_all[b]
        for copy in sums + shares:
            copy.wait_send()

    with jax.named_scope("drain"):
        for ex in coef_ex + grad_ex:
            ex.drain()
        for gather in gathers:
            gather.drain()
        for copy in pairs + [c for some in scatters for c in some]:
            copy.wait_send()


def widen(inc, grad, inc_out, grad_out):
    inc_out[...] = inc[...].astype(F32)
    grad_out[...] = grad[...].astype(F32)


def on_device(zn, sn, anomalies, alpha, basis, gradient, vertical_root, band_gain, band, order):
    members, levels, columns = anomalies.shape
    modes = alpha.shape[2]
    rows = members * levels
    qn = sn // 2
    slots = zn * members
    gw = min(LANES, modes)
    groups = modes // gw
    lv = levels // HALVES
    parts = HALVES * groups
    arrivals = 2 if qn == 4 else qn - 1
    width = columns // STRIPS
    line = zn == 4
    vmem = pl.BlockSpec(memory_space=pltpu.VMEM)
    smem = pl.BlockSpec(memory_space=pltpu.SMEM)
    hbm = pl.BlockSpec(memory_space=pl.ANY)
    dma = pltpu.SemaphoreType.DMA
    lookup = (1, -(-slots // LANES) * LANES)
    scratch = dict(
        anom=pltpu.VMEM((members, levels, columns), BF16),
        base=pltpu.VMEM((sn, modes, columns), BF16),
        weighted=pltpu.VMEM((rows, columns), BF16),
        alpha=pltpu.VMEM((rows, modes), BF16),
        gradient=pltpu.VMEM((levels, columns), BF16),
        vroot=pltpu.VMEM((levels, levels), F32),
        band=pltpu.VMEM((modes,), jnp.int32),
        gain=pltpu.VMEM((1, modes), F32),
        root_t=pltpu.VMEM((2, GROUP, GROUP), BF16),
        inv_v=pltpu.VMEM(lookup, jnp.int32),
        inv_s=pltpu.SMEM(lookup, jnp.int32),
        coef_pack=pltpu.VMEM((parts, members * lv, gw), BF16),
        pick=pltpu.VMEM((parts, sn, members * lv, gw), BF16),
        pair_out=pltpu.VMEM((groups * qn, rows, gw), F32),
        pair_in=pltpu.VMEM((groups * qn, rows, gw), F32),
        mine=pltpu.VMEM((groups * qn, rows, gw), F32),
        rs_out=pltpu.VMEM((groups, qn - 1, rows, gw), BF16),
        rs_in=pltpu.VMEM((groups, arrivals, rows, gw), BF16),
        relay_in=pltpu.VMEM((groups, rows, gw), BF16),
        grad_pack=pltpu.VMEM((groups, rows, gw), BF16),
        got=pltpu.VMEM((groups, rows, gw), BF16),
        acc=pltpu.VMEM((members * lv, columns), F32),
        inc_part=pltpu.VMEM((levels, columns), F32),
        load_sem=dma((5,)),
        base_sem=dma((groups * sn,)),
        inv_sem=dma,
        z_send=dma((parts, zn)),
        z_recv=dma((parts, zn)),
        g_send=dma((groups, zn)),
        g_recv=dma((groups, zn)),
        pk_send=dma((parts, sn)),
        pk_recv=dma((parts, sn)),
        pair_send=dma((groups * qn,)),
        pair_recv=dma((groups * qn,)),
        rs_send=dma((groups, qn - 1)),
        rs_recv=dma((groups, qn - 1)),
    )
    scratch |= {f"coef_held{p}": pltpu.VMEM((slots, lv, gw), BF16) for p in range(parts)}
    scratch |= {f"grad_held{g}": pltpu.VMEM((slots, levels, gw), BF16) for g in range(groups)}
    if line:
        strips = (HALVES, STRIPS, lv, width)
        scratch |= {n: pltpu.VMEM(strips, BF16) for n in ("inc_out", "inc_in", "inc_sum", "inc_got", "inc_all")}
        signals = ("is_send", "is_recv", "ic_send", "ic_recv", "if_send", "if_recv")
        scratch |= {n: dma((HALVES, STRIPS)) for n in signals}
    else:
        strips = (zn, levels, columns // zn)
        scratch |= {n: pltpu.VMEM(strips, BF16) for n in ("inc_out", "inc_in", "inc_all")}
        scratch |= {n: dma((zn,)) for n in ("is_send", "is_recv", "if_send", "if_recv")}
    increment, grads = pl.pallas_call(
        functools.partial(kernel, zn, sn, tuple(scratch)),
        out_shape=(
            jax.ShapeDtypeStruct((levels, columns), BF16),
            jax.ShapeDtypeStruct((rows, modes), BF16),
        ),
        in_specs=[smem] * 2 + [hbm] * 6,
        out_specs=(vmem, vmem),
        scratch_shapes=list(scratch.values()),
        compiler_params=pltpu.CompilerParams(
            collective_id=0, has_side_effects=True, vmem_limit_bytes=58 * 2**20
        ),
    )(
        order, band_gain, vertical_root, alpha.reshape(rows, modes), band, gradient,
        anomalies, basis.reshape(sn, modes, columns),
    )
    increment, grads = pl.pallas_call(
        widen,
        out_shape=(
            jax.ShapeDtypeStruct((levels, columns), F32),
            jax.ShapeDtypeStruct((rows, modes), F32),
        ),
        in_specs=[vmem] * 2,
        out_specs=(vmem, vmem),
    )(increment, grads)
    return increment, grads.reshape(members, levels, modes)


def solution(mesh):
    zn, sn = mesh.shape["mem"], mesh.shape["state"]
    return jax.shard_map(
        functools.partial(on_device, zn, sn),
        mesh=mesh,
        in_specs=(
            P("mem", None, "state"),
            P("mem", None, "state"),
            P(None, "state"),
            P(None, "state"),
            P(),
            P(),
            P("state"),
            P(),
        ),
        out_specs=(P(None, "state"), P("mem", None, "state")),
        check_vma=False,
    )
```

```python
import functools
import types
import jax
import jax.numpy as jnp
from jax import lax
from jax.experimental import pallas as pl
from jax.experimental.pallas import tpu as pltpu
from jax.sharding import PartitionSpec as P

MESH = pl.DeviceIdType.MESH
F32 = jnp.float32
BF16 = jnp.bfloat16
NT = (((1,), (1,)), ((), ()))
LANES = 128
GROUP = 256
HALVES = 2
STRIPS = 4


def flip(a, k, n):
    out, bit, k = 0, 1, jnp.asarray(k, jnp.int32)
    while bit < n:
        out = out + lax.rem(lax.div(a, bit) + lax.div(k, bit), 2) * bit
        bit *= 2
    return out


def split(v):
    high = v.astype(BF16)
    return high, (v - high.astype(F32)).astype(BF16)


def kernel(
    zn, sn, names,
    order, band_gain, vroot_h, alpha_h, band_h, gradient_h, anomalies, basis,
    inc_out, grad_out, *scratch,
):
    r = types.SimpleNamespace(**dict(zip(names, scratch)))
    coef_held = [ref for name, ref in zip(names, scratch) if name.startswith("coef_held")]
    grad_held = [ref for name, ref in zip(names, scratch) if name.startswith("grad_held")]
    z = lax.axis_index("mem")
    s = lax.axis_index("state")
    chip, core = lax.div(s, 2), lax.rem(s, 2)
    qn = sn // 2
    partner = chip * 2 + (1 - core)
    members, levels, columns = r.anom.shape
    modes = r.alpha.shape[1]
    parts = len(coef_held)
    _, lv, gw = coef_held[0].shape
    groups = modes // gw
    rows = members * levels
    slots = zn * members
    width = columns // STRIPS
    line, square = zn == 4, qn == 4
    tuned = line and square and groups == 2

    zpeer = [flip(z, k, zn) for k in range(zn)]
    qpeer = [flip(chip, k, qn) for k in range(qn)]
    if square:
        first = qpeer[1] * (1 - core) + qpeer[2] * core
        second = qpeer[2] * (1 - core) + qpeer[1] * core

    def chip_at(i, side):
        if square:
            i = side * i + (1 - side) * (lax.rem(i, 2) * 2 + lax.div(i, 2))
        return flip(chip, qn - 1 - i, qn)

    def own_block(i):
        return chip_at(i, core) * 2 + core

    def other_block(i):
        return chip_at(i, 1 - core) * 2 + 1 - core

    small = [
        pltpu.make_async_copy(src, dst, r.load_sem.at[i])
        for i, (src, dst) in enumerate(
            [(vroot_h, r.vroot), (alpha_h, r.alpha), (band_h, r.band), (gradient_h, r.gradient), (anomalies, r.anom)]
        )
    ]
    for copy in small:
        copy.start()

    barrier = pltpu.get_barrier_semaphore()
    for k in range(1, zn):
        pl.semaphore_signal(barrier, inc=1, device_id={"mem": zpeer[k]}, device_id_type=MESH)
    for k in range(1, qn):
        pl.semaphore_signal(barrier, inc=1, device_id={"state": qpeer[k] * 2 + core}, device_id_type=MESH)
    pl.semaphore_signal(barrier, inc=1, device_id={"state": partner}, device_id_type=MESH)

    def mode_rows(g):
        return pl.ds(pl.multiple_of(g * gw, gw), gw)

    def load_of(g, t, n):
        here = mode_rows(g)
        return pltpu.make_async_copy(basis.at[t, here], r.base.at[t, here], r.base_sem.at[n])

    def loads_of(n):
        i, g = lax.div(n, groups), lax.rem(n, groups)
        return load_of(g, other_block(i), 2 * n), load_of(g, own_block(i), 2 * n + 1)

    units = groups * qn

    def to(src, dst, send, recv, **where):
        return pltpu.make_async_remote_copy(
            src_ref=src, dst_ref=dst, send_sem=send, recv_sem=recv, device_id=where, device_id_type=MESH
        )

    spot = lax.broadcasted_iota(jnp.int32, r.inv_v.shape, 1)
    inverse = jnp.zeros(r.inv_v.shape, jnp.int32)
    for j in range(slots):
        inverse = jnp.where(spot == order[j], j, inverse)
    r.inv_v[...] = inverse
    inv_copy = pltpu.make_async_copy(r.inv_v, r.inv_s, r.inv_sem)
    inv_copy.start()

    own_rows = pl.ds(z * members, members)
    outer = lax.div(lax.rem(z + 1, zn), 2) == 0
    inner = jnp.logical_not(outer)
    near = 1 + lax.div(z, 2)
    mid = 3 - near
    other = 3 - z
    rim = (z - 1) * 3
    distant = 3 - rim

    class Exchange:
        def __init__(self, find, held, pack, mine, height, send, recv):
            self.find, self.held, self.pack, self.mine, self.height = find, held, pack, mine, height
            own = held.at[own_rows]
            if not line:
                self.out = [to(own, own, send.at[k], recv.at[z], mem=zpeer[k]) for k in range(1, zn)]
                self.come = [self.arrival(zpeer[k], send, recv, zpeer[k]) for k in range(1, zn)]
                return
            self.to_mid = to(own, own, send.at[0], recv.at[z], mem=mid)
            self.to_near = to(own, own, send.at[1], recv.at[z], mem=near)
            self.to_other = to(own, own, send.at[0], recv.at[z], mem=other)
            self.give = to(pack, mine, send.at[2], recv.at[z], mem=rim)
            self.given = to(pack, mine, send.at[2], recv.at[near], mem=near)
            self.come = [self.arrival(a, send, recv, other) for a in (rim, other, distant)]

        def arrival(self, a, send, recv, where):
            there = self.held.at[pl.ds(a * members, members)]
            return to(there, there, send.at[0], recv.at[a], mem=where)

        def start(self):
            if not line:
                for copy in self.out:
                    copy.start()
                return

            @pl.when(outer)
            def _():
                self.to_mid.start()
                self.to_near.start()

            @pl.when(inner)
            def _():
                self.to_other.start()

        def choose(self, out, who):
            for m in range(members):
                out[m * self.height : (m + 1) * self.height, :] = self.held[self.find(who * members + m)]

        def take_inner(self):
            for copy in self.come:
                copy.wait_recv()
            self.choose(self.pack, rim)
            self.give.start()
            self.choose(self.mine, z)

        def take_outer(self):
            self.given.wait_recv()

        def take(self):
            for copy in self.come:
                copy.wait_recv()
            self.choose(self.mine, z)

        def drain(self):
            if not line:
                for copy in self.out:
                    copy.wait_send()
                return

            @pl.when(outer)
            def _():
                self.to_mid.wait_send()
                self.to_near.wait_send()

            @pl.when(inner)
            def _():
                self.to_other.wait_send()
                self.give.wait_send()

    grid = (GROUP, levels)
    row_of = lax.broadcasted_iota(jnp.int32, grid, 0)
    level_of = lax.broadcasted_iota(jnp.int32, grid, 1)
    chunk = GROUP // HALVES
    piece_level = lax.div(row_of, chunk) * lv + lax.rem(row_of, lv)
    plain = jnp.where(lax.rem(row_of, levels) == level_of, 1.0, 0.0).astype(BF16)
    pieced = jnp.where(piece_level == level_of, 1.0, 0.0).astype(BF16)
    wide = (GROUP, GROUP)
    here_of = lax.broadcasted_iota(jnp.int32, wide, 0)
    there_of = lax.div(lax.broadcasted_iota(jnp.int32, wide, 1), levels)
    same_plain = lax.div(here_of, levels) == there_of
    same_pieced = lax.div(lax.rem(here_of, chunk), lv) == there_of

    def dot(a, b):
        return jnp.dot(a, b, preferred_element_type=F32)

    def dot_nt(a, b):
        return lax.dot_general(a, b, NT, preferred_element_type=F32)

    def blocks(tall, same):
        full = dot_nt(tall.astype(BF16), plain)
        return jnp.where(same, full, 0.0).astype(BF16)

    with jax.named_scope("coef"):
        small[0].wait()
        root_terms = split(r.vroot[...])
        root = [blocks(dot(pieced, v), same_pieced) for v in root_terms]
        root_t = [blocks(dot_nt(plain, v), same_plain) for v in root_terms]
        for v, keep in zip(root_t, (0, 1)):
            r.root_t[keep] = v
        small[1].wait()
        small[2].wait()

        def load(n, carry):
            for copy in loads_of(n):
                copy.start()
            return carry

        lax.fori_loop(0, units, load, 0)
        band = r.band[...].reshape(1, modes)
        gain = jnp.zeros((1, modes), F32)
        for b in range(band_gain.shape[0]):
            gain = jnp.where(band == b, band_gain[b], gain)
        r.gain[...] = gain
        for n in range(rows // GROUP):
            control = r.alpha[n * GROUP : (n + 1) * GROUP, :]
            coef = (dot(root[0], control) + dot(root[1], control)) * gain
            coef = coef.astype(BF16)
            count = GROUP // levels
            for c in range(HALVES):
                for g in range(groups):
                    block = coef[c * chunk : (c + 1) * chunk, g * gw : (g + 1) * gw]
                    at = pl.ds(z * members + n * count, count)
                    coef_held[c * groups + g][at] = block.reshape(count, lv, gw)
    with jax.named_scope("barrier"):
        pl.semaphore_wait(barrier, zn - 1 + qn)

    coef_ex = [
        Exchange(
            lambda m: r.inv_s[0, m], coef_held[p], r.coef_pack.at[p], r.pick.at[p, s], lv,
            r.z_send.at[p], r.z_recv.at[p],
        )
        for p in range(parts)
    ]
    for ex in coef_ex:
        ex.start()
    grad_ex = [
        Exchange(
            lambda m: order[m], grad_held[g], r.grad_pack.at[g], r.got.at[g], levels,
            r.g_send.at[g], r.g_recv.at[g],
        )
        for g in range(groups)
    ]

    with jax.named_scope("weigh"):
        small[3].wait()
        small[4].wait()

        def weigh(m, carry):
            at = pl.ds(pl.multiple_of(m * levels, levels), levels)
            r.weighted[at, :] = (r.anom[m].astype(F32) * r.gradient[...].astype(F32)).astype(BF16)
            return carry

        lax.fori_loop(0, members, weigh, 0)

    def block_of(p, t):
        return r.pick.at[p, t]

    def share(p, t, i, where):
        return to(block_of(p, t), block_of(p, t), r.pk_send.at[p, i], r.pk_recv.at[p, t], state=where)

    class Gather:
        def __init__(self, p):
            there = [qpeer[k] * 2 + core for k in range(1, qn)]
            self.out = [share(p, s, i, where) for i, where in enumerate(there)]
            self.out.append(share(p, s, qn - 1, partner))
            self.over = [share(p, t, qn + i, partner) for i, t in enumerate(there)]
            self.rest = [share(p, qpeer[k] * 2 + 1 - core, 0, partner) for k in range(qn)]

        def start(self):
            for copy in self.out:
                copy.start()

        def pass_on(self):
            for copy in self.over:
                copy.wait_recv()
                copy.start()

        def finish(self):
            for copy in self.rest:
                copy.wait_recv()

        def drain(self):
            for copy in self.out + self.over:
                copy.wait_send()

    gathers = [Gather(p) for p in range(parts)]

    def on_inner(*fns):
        def run():
            for fn in fns:
                fn()

        if line:
            pl.when(inner)(run)

    def on_outer(*fns):
        def run():
            for fn in fns:
                fn()

        if line:
            pl.when(outer)(run)

    def pair_of(n):
        return to(r.pair_out.at[n], r.pair_in.at[n], r.pair_send.at[n], r.pair_recv.at[n], state=partner)

    def scatter(g, i, dst, where):
        n = i * groups + g
        return to(r.rs_out.at[n], dst, r.rs_send.at[n], r.rs_recv.at[n], state=where * 2 + core)

    def scatters_of(g):
        if not square:
            return [scatter(g, i, r.rs_in.at[g * (qn - 1) + i], chip_at(i, core)) for i in range(qn - 1)]
        return [
            scatter(g, 0, r.relay_in.at[g], first),
            scatter(g, 1, r.rs_in.at[g * 2], first),
            scatter(g, 2, r.rs_in.at[g * 2 + 1], second),
        ]

    def combine(n):
        i, g = lax.div(n, groups), lax.rem(n, groups)
        pair_of(n).wait_recv()

        @pl.when(i == qn - 1)
        def _():
            r.mine[n] = r.mine[n] + r.pair_in[n]

        copies = scatters_of(g)
        for k, copy in enumerate(copies):

            @pl.when(i == k)
            def _():
                total = r.mine[n] + r.pair_in[n]
                if square and k == 2:
                    copies[0].wait_recv()
                    total = total + r.relay_in[g].astype(F32)
                r.rs_out[n] = total.astype(BF16)
                copy.start()

    def adjoint(g):
        scatters = scatters_of(g)[1:] if square else scatters_of(g)
        for copy in scatters:
            copy.wait_recv()
        total = r.mine[(qn - 1) * groups + g]
        for i in range(len(scatters)):
            total = total + r.rs_in[g * len(scatters) + i].astype(F32)
        stack = jnp.concatenate([total[n * GROUP : (n + 1) * GROUP] for n in range(rows // GROUP)], axis=1)
        high, low = split(stack)
        grad = dot(r.root_t[0], high) + dot(r.root_t[0], low) + dot(r.root_t[1], high)
        scale = r.gain[:, g * gw : (g + 1) * gw]
        count = GROUP // levels
        for n in range(rows // GROUP):
            block = (grad[:, n * gw : (n + 1) * gw] * scale).astype(BF16)
            grad_held[g][pl.ds(z * members + n * count, count)] = block.reshape(count, levels, gw)
        grad_ex[g].start()

    inv_copy.wait()
    take_in = [ex.take_inner for ex in coef_ex] if line else []
    take_out = [ex.take_outer for ex in coef_ex] if line else []
    services = {
        2: lambda: on_inner(take_in[0]),
        4: lambda: on_inner(take_in[1]),
        6: lambda: on_inner(take_in[2]),
    }

    def unit(n, carry):
        i = lax.div(n, groups)
        cut = mode_rows(lax.rem(n, groups))
        for copy in loads_of(n):
            copy.wait()
        with jax.named_scope("unit"):
            rhs = jnp.concatenate([r.base[other_block(i), cut, :], r.base[own_block(i), cut, :]], axis=0)
            both = dot_nt(r.weighted[...], rhs)
            r.pair_out[n] = both[:, :gw]
            r.mine[n] = both[:, gw:]
        pair_of(n).start()

        @pl.when(n > 0)
        def _():
            combine(n - 1)

        if tuned:
            for at, serve in services.items():
                pl.when(n == at)(serve)
        return carry

    lax.fori_loop(0, units, unit, 0)
    if line:
        def stage_of(c, j):
            return to(r.inc_out.at[c, j], r.inc_in.at[c, j], r.is_send.at[c, j], r.is_recv.at[c, j], mem=near)

        def cross_of(c, j):
            return to(r.inc_sum.at[c, j], r.inc_got.at[c, j], r.ic_send.at[c, j], r.ic_recv.at[c, j], mem=other)

        def final_of(c, j, where):
            return to(r.inc_all.at[c, j], r.inc_all.at[c, j], r.if_send.at[c, j], r.if_recv.at[c, j], mem=where)

    def spread(c, g, hooks={}):
        p = c * groups + g

        def part(j, carry):
            at = pl.ds(pl.multiple_of(j * width, width), width)
            cut = slice(g * gw, (g + 1) * gw)
            lhs = jnp.concatenate([r.pick[p, t] for t in range(sn)], axis=1)
            rhs = jnp.concatenate([r.base[t, cut, at] for t in range(sn)], axis=0)
            field = dot(lhs, rhs)
            if g > 0:
                field = field + r.acc[:, at]
            for k, hook in hooks.items():
                pl.when(j == k)(hook)
            if g < groups - 1:
                r.acc[:, at] = field
                return carry
            run = jnp.zeros((lv, width), F32)
            for m in range(members):
                run = run + field[m * lv : (m + 1) * lv] * r.anom[m, c * lv : (c + 1) * lv, at].astype(F32)
            r.inc_part[c * lv : (c + 1) * lv, at] = run
            if line:

                @pl.when(outer)
                def _():
                    r.inc_out[c, j] = run.astype(BF16)
                    stage_of(c, j).start()

            return carry

        lax.fori_loop(0, STRIPS, part, 0)

    def each(fn):
        def step(j, carry):
            fn(j)
            return carry

        lax.fori_loop(0, STRIPS, step, 0)

    def inner_sum(c):
        def one(j):
            at = pl.ds(pl.multiple_of(j * width, width), width)
            stage_of(c, j).wait_recv()
            total = r.inc_part[c * lv : (c + 1) * lv, at] + r.inc_in[c, j].astype(F32)
            r.inc_sum[c, j] = total.astype(BF16)
            cross_of(c, j).start()

        if line:
            @pl.when(inner)
            def _():
                each(one)

    def inner_final(c):
        def one(j):
            cross_of(c, j).wait_recv()
            total = r.inc_sum[c, j].astype(F32) + r.inc_got[c, j].astype(F32)
            r.inc_all[c, j] = total.astype(BF16)
            final_of(c, j, rim).start()

        if line:
            @pl.when(inner)
            def _():
                each(one)

    def grad_inner(g):
        if line and g < groups:

            @pl.when(inner)
            def _():
                grad_ex[g].take_inner()

    def scoped(name, *fns):
        with jax.named_scope(name):
            for fn in fns:
                fn()

    if tuned:
        scoped("start0", lambda: on_outer(take_out[0]), gathers[0].start)
        scoped("inner3", lambda: on_inner(take_in[3], gathers[1].start))
        scoped("combine", lambda: combine(jnp.int32(units - 1)))
        scoped("adjoint0", lambda: adjoint(0))
        scoped("start1", lambda: on_outer(take_out[1], gathers[1].start))
        scoped("adjoint1", lambda: adjoint(1))
        scoped("start2", lambda: on_outer(take_out[2]), gathers[2].start)
        scoped("pass0", gathers[0].pass_on)
        scoped("fin0", gathers[0].finish)
        scoped("spread0", lambda: spread(0, 0, {
            0: lambda: on_inner(gathers[3].start),
            1: lambda: on_outer(take_out[3], gathers[3].start),
            2: gathers[1].pass_on,
        }))
        scoped("fin1", gathers[1].finish)
        scoped("spread1", lambda: spread(0, 1, {2: gathers[2].pass_on}))
        scoped("grad0", lambda: grad_inner(0))
        scoped("fin2", gathers[2].finish)
        scoped("spread2", lambda: spread(1, 0, {2: gathers[3].pass_on, 3: lambda: inner_sum(0)}))
        scoped("grad1", lambda: grad_inner(1))
        scoped("fin3", gathers[3].finish)
        scoped("spread3", lambda: spread(1, 1, {3: lambda: inner_final(0)}))
        scoped("sum1", lambda: inner_sum(1))
        scoped("final1", lambda: inner_final(1))
    else:
        combine(jnp.int32(units - 1))
        for p in range(parts):
            if line:
                on_inner(take_in[p])
                on_outer(take_out[p])
            else:
                coef_ex[p].take()
            gathers[p].start()
        for g in range(groups):
            adjoint(g)
        for c in range(HALVES):
            for g in range(groups):
                gathers[c * groups + g].pass_on()
                gathers[c * groups + g].finish()
                spread(c, g)
            inner_sum(c)
            inner_final(c)
        for g in range(groups):
            grad_inner(g)

    with jax.named_scope("settle"):
        if line:
            @pl.when(outer)
            def _():
                for ex in grad_ex:
                    ex.take_outer()
        else:
            for ex in grad_ex:
                ex.take()
        for g in range(groups):
            grad_out[:, g * gw : (g + 1) * gw] = r.got[g]

    if line:
        with jax.named_scope("last"):
            @pl.when(outer)
            def _():
                for c in range(HALVES):
                    each(lambda j, c=c: final_of(c, j, near).wait_recv())

            for c in range(HALVES):
                for j in range(STRIPS):
                    inc_out[c * lv : (c + 1) * lv, j * width : (j + 1) * width] = r.inc_all[c, j]

        @pl.when(outer)
        def _():
            for c in range(HALVES):
                each(lambda j, c=c: stage_of(c, j).wait_send())

        @pl.when(inner)
        def _():
            for c in range(HALVES):
                each(lambda j, c=c: cross_of(c, j).wait_send())
                each(lambda j, c=c: final_of(c, j, rim).wait_send())
    else:
        strip = columns // zn
        sums = [
            to(r.inc_out.at[k], r.inc_in.at[k], r.is_send.at[k], r.is_recv.at[k], mem=zpeer[k]) for k in range(1, zn)
        ]
        for k in range(1, zn):
            at = pl.ds(pl.multiple_of(zpeer[k] * strip, strip), strip)
            r.inc_out[k] = r.inc_part[:, at].astype(BF16)
            sums[k - 1].start()
        run = r.inc_part[:, pl.ds(pl.multiple_of(z * strip, strip), strip)]
        for k in range(1, zn):
            sums[k - 1].wait_recv()
            run = run + r.inc_in[k].astype(F32)
        r.inc_all[z] = run.astype(BF16)

        def held(k, a):
            return to(r.inc_all.at[a], r.inc_all.at[a], r.if_send.at[k], r.if_recv.at[a], mem=zpeer[k])

        shares = [held(k, z) for k in range(1, zn)]
        for copy in shares:
            copy.start()
        for k in range(1, zn):
            held(k, zpeer[k]).wait_recv()
        for b in range(zn):
            inc_out[:, b * strip : (b + 1) * strip] = r.inc_all[b]
        for copy in sums + shares:
            copy.wait_send()

    with jax.named_scope("drain"):
        for ex in coef_ex + grad_ex:
            ex.drain()
        for gather in gathers:
            gather.drain()
        for n in range(units):
            pair_of(n).wait_send()
        for g in range(groups):
            for copy in scatters_of(g):
                copy.wait_send()


def widen(inc, grad, inc_out, grad_out):
    inc_out[...] = inc[...].astype(F32)
    grad_out[...] = grad[...].astype(F32)


def on_device(zn, sn, anomalies, alpha, basis, gradient, vertical_root, band_gain, band, order):
    members, levels, columns = anomalies.shape
    modes = alpha.shape[2]
    rows = members * levels
    qn = sn // 2
    slots = zn * members
    gw = min(LANES, modes)
    groups = modes // gw
    lv = levels // HALVES
    parts = HALVES * groups
    arrivals = 2 if qn == 4 else qn - 1
    width = columns // STRIPS
    line = zn == 4
    vmem = pl.BlockSpec(memory_space=pltpu.VMEM)
    smem = pl.BlockSpec(memory_space=pltpu.SMEM)
    hbm = pl.BlockSpec(memory_space=pl.ANY)
    dma = pltpu.SemaphoreType.DMA
    lookup = (1, -(-slots // LANES) * LANES)
    scratch = dict(
        anom=pltpu.VMEM((members, levels, columns), BF16),
        base=pltpu.VMEM((sn, modes, columns), BF16),
        weighted=pltpu.VMEM((rows, columns), BF16),
        alpha=pltpu.VMEM((rows, modes), BF16),
        gradient=pltpu.VMEM((levels, columns), BF16),
        vroot=pltpu.VMEM((levels, levels), F32),
        band=pltpu.VMEM((modes,), jnp.int32),
        gain=pltpu.VMEM((1, modes), F32),
        root_t=pltpu.VMEM((2, GROUP, GROUP), BF16),
        inv_v=pltpu.VMEM(lookup, jnp.int32),
        inv_s=pltpu.SMEM(lookup, jnp.int32),
        coef_pack=pltpu.VMEM((parts, members * lv, gw), BF16),
        pick=pltpu.VMEM((parts, sn, members * lv, gw), BF16),
        pair_out=pltpu.VMEM((groups * qn, rows, gw), F32),
        pair_in=pltpu.VMEM((groups * qn, rows, gw), F32),
        mine=pltpu.VMEM((groups * qn, rows, gw), F32),
        rs_out=pltpu.VMEM((groups * qn, rows, gw), BF16),
        rs_in=pltpu.VMEM((groups * arrivals, rows, gw), BF16),
        relay_in=pltpu.VMEM((groups, rows, gw), BF16),
        grad_pack=pltpu.VMEM((groups, rows, gw), BF16),
        got=pltpu.VMEM((groups, rows, gw), BF16),
        acc=pltpu.VMEM((members * lv, columns), F32),
        inc_part=pltpu.VMEM((levels, columns), F32),
        load_sem=dma((5,)),
        base_sem=dma((groups * sn,)),
        inv_sem=dma,
        z_send=dma((parts, zn)),
        z_recv=dma((parts, zn)),
        g_send=dma((groups, zn)),
        g_recv=dma((groups, zn)),
        pk_send=dma((parts, sn)),
        pk_recv=dma((parts, sn)),
        pair_send=dma((groups * qn,)),
        pair_recv=dma((groups * qn,)),
        rs_send=dma((groups * qn,)),
        rs_recv=dma((groups * qn,)),
    )
    scratch |= {f"coef_held{p}": pltpu.VMEM((slots, lv, gw), BF16) for p in range(parts)}
    scratch |= {f"grad_held{g}": pltpu.VMEM((slots, levels, gw), BF16) for g in range(groups)}
    if line:
        strips = (HALVES, STRIPS, lv, width)
        scratch |= {n: pltpu.VMEM(strips, BF16) for n in ("inc_out", "inc_in", "inc_sum", "inc_got", "inc_all")}
        signals = ("is_send", "is_recv", "ic_send", "ic_recv", "if_send", "if_recv")
        scratch |= {n: dma((HALVES, STRIPS)) for n in signals}
    else:
        strips = (zn, levels, columns // zn)
        scratch |= {n: pltpu.VMEM(strips, BF16) for n in ("inc_out", "inc_in", "inc_all")}
        scratch |= {n: dma((zn,)) for n in ("is_send", "is_recv", "if_send", "if_recv")}
    increment, grads = pl.pallas_call(
        functools.partial(kernel, zn, sn, tuple(scratch)),
        out_shape=(
            jax.ShapeDtypeStruct((levels, columns), BF16),
            jax.ShapeDtypeStruct((rows, modes), BF16),
        ),
        in_specs=[smem] * 2 + [hbm] * 6,
        out_specs=(vmem, vmem),
        scratch_shapes=list(scratch.values()),
        compiler_params=pltpu.CompilerParams(
            collective_id=0, has_side_effects=True, vmem_limit_bytes=58 * 2**20
        ),
    )(
        order, band_gain, vertical_root, alpha.reshape(rows, modes), band, gradient,
        anomalies, basis.reshape(sn, modes, columns),
    )
    increment, grads = pl.pallas_call(
        widen,
        out_shape=(
            jax.ShapeDtypeStruct((levels, columns), F32),
            jax.ShapeDtypeStruct((rows, modes), F32),
        ),
        in_specs=[vmem] * 2,
        out_specs=(vmem, vmem),
    )(increment, grads)
    return increment, grads.reshape(members, levels, modes)


def solution(mesh):
    zn, sn = mesh.shape["mem"], mesh.shape["state"]
    return jax.shard_map(
        functools.partial(on_device, zn, sn),
        mesh=mesh,
        in_specs=(
            P("mem", None, "state"),
            P("mem", None, "state"),
            P(None, "state"),
            P(None, "state"),
            P(),
            P(),
            P("state"),
            P(),
        ),
        out_specs=(P(None, "state"), P("mem", None, "state")),
        check_vma=False,
    )
```

```python
import functools
import types
import jax
import jax.numpy as jnp
from jax import lax
from jax.experimental import pallas as pl
from jax.experimental.pallas import tpu as pltpu
from jax.sharding import PartitionSpec as P

MESH = pl.DeviceIdType.MESH
F32 = jnp.float32
BF16 = jnp.bfloat16
NT = (((1,), (1,)), ((), ()))
LANES = 128
GROUP = 256
HALVES = 2
STRIPS = 4


def flip(a, k, n):
    out, bit, k = 0, 1, jnp.asarray(k, jnp.int32)
    while bit < n:
        out = out + lax.rem(lax.div(a, bit) + lax.div(k, bit), 2) * bit
        bit *= 2
    return out


def split(v):
    high = v.astype(BF16)
    return high, (v - high.astype(F32)).astype(BF16)


def kernel(
    zn, sn, names,
    order_h, band_gain_h, vroot_h, alpha_h, band_h, gradient_h, anomalies, basis,
    inc_out, grad_out, *scratch,
):
    r = types.SimpleNamespace(**dict(zip(names, scratch)))
    coef_held = [ref for name, ref in zip(names, scratch) if name.startswith("coef_held")]
    grad_held = [ref for name, ref in zip(names, scratch) if name.startswith("grad_held")]
    z = lax.axis_index("mem")
    s = lax.axis_index("state")
    chip, core = lax.div(s, 2), lax.rem(s, 2)
    qn = sn // 2
    partner = chip * 2 + (1 - core)
    members, levels, columns = r.anom.shape
    modes = r.alpha.shape[1]
    parts = len(coef_held)
    _, lv, gw = coef_held[0].shape
    groups = modes // gw
    rows = members * levels
    slots = zn * members
    width = columns // STRIPS
    line, square = zn == 4, qn == 4
    tuned = line and square and groups == 2

    zpeer = [flip(z, k, zn) for k in range(zn)]
    qpeer = [flip(chip, k, qn) for k in range(qn)]
    if square:
        first = qpeer[1] * (1 - core) + qpeer[2] * core
        second = qpeer[2] * (1 - core) + qpeer[1] * core

    def chip_at(i, side):
        if square:
            i = side * i + (1 - side) * (lax.rem(i, 2) * 2 + lax.div(i, 2))
        return flip(chip, qn - 1 - i, qn)

    def own_block(i):
        return chip_at(i, core) * 2 + core

    def other_block(i):
        return chip_at(i, 1 - core) * 2 + 1 - core

    small = [
        pltpu.make_async_copy(src, dst, r.load_sem.at[i])
        for i, (src, dst) in enumerate(
            [
                (vroot_h, r.vroot), (alpha_h, r.alpha), (band_h, r.band), (band_gain_h, r.band_gain),
                (order_h, r.order), (gradient_h, r.gradient), (anomalies, r.anom),
            ]
        )
    ]
    for copy in small:
        copy.start()

    barrier = pltpu.get_barrier_semaphore()
    for k in range(1, zn):
        pl.semaphore_signal(barrier, inc=1, device_id={"mem": zpeer[k]}, device_id_type=MESH)
    for k in range(1, qn):
        pl.semaphore_signal(barrier, inc=1, device_id={"state": qpeer[k] * 2 + core}, device_id_type=MESH)
    pl.semaphore_signal(barrier, inc=1, device_id={"state": partner}, device_id_type=MESH)

    def mode_rows(g):
        return pl.ds(pl.multiple_of(g * gw, gw), gw)

    def load_of(g, t, n):
        here = mode_rows(g)
        return pltpu.make_async_copy(basis.at[t, here], r.base.at[t, here], r.base_sem.at[n])

    def loaded(n):
        two = (pl.ds(0, 2), pl.ds(0, gw))
        return pltpu.make_async_copy(basis.at[two], r.base.at[two], r.base_sem.at[n])

    def loads_of(n):
        i, g = lax.div(n, groups), lax.rem(n, groups)
        return load_of(g, other_block(i), n), load_of(g, own_block(i), n)

    units = groups * qn

    def to(src, dst, send, recv, **where):
        return pltpu.make_async_remote_copy(
            src_ref=src, dst_ref=dst, send_sem=send, recv_sem=recv, device_id=where, device_id_type=MESH
        )

    own_rows = pl.ds(z * members, members)
    outer = lax.div(lax.rem(z + 1, zn), 2) == 0
    inner = jnp.logical_not(outer)
    near = 1 + lax.div(z, 2)
    mid = 3 - near
    other = 3 - z
    rim = (z - 1) * 3
    distant = 3 - rim

    class Exchange:
        def __init__(self, find, held, pack, mine, height, send, recv, rim_recv=None):
            self.find, self.held, self.pack, self.mine, self.height = find, held, pack, mine, height
            own = held.at[own_rows]
            come = held.at[pl.ds(0, (zn - 1) * members)]
            self.come = to(come, come, send, recv, mem=zpeer[1])
            gone = held.at[pl.ds(0, (2 if line else zn - 1) * members)]
            self.gone = to(gone, gone, send, recv, mem=zpeer[1])
            self.relayed, self.send = rim_recv is not None, send
            if not line:
                self.out = [to(own, own, send, recv, mem=zpeer[k]) for k in range(1, zn)]
                return
            self.to_mid = to(own, own, send, recv, mem=mid)
            self.to_near = to(own, own, send, rim_recv if self.relayed else recv, mem=near)
            self.to_other = to(own, own, send, recv, mem=other)
            if self.relayed:
                rims = held.at[pl.ds(rim * members, members)]
                self.from_rim = to(rims, rims, send, rim_recv, mem=other)
                self.hand_on = to(rims, rims, send, recv, mem=other)
                count = pl.ds(0, 2 * members)
                self.come = to(held.at[count], held.at[count], send, recv, mem=other)
            self.give = to(pack, mine, send, recv, mem=rim)
            self.given = to(pack, mine, send, recv, mem=near)

        def start(self):
            if not line:
                for copy in self.out:
                    copy.start()
                return

            @pl.when(outer)
            def _():
                if not self.relayed:
                    self.to_mid.start()
                self.to_near.start()

            @pl.when(inner)
            def _():
                self.to_other.start()

        def choose(self, out, who):
            for m in range(members):
                out[m * self.height : (m + 1) * self.height, :] = self.held[self.find(who * members + m)]

        def take_inner(self):
            self.come.wait_recv()
            self.choose(self.pack, rim)
            self.give.start()
            self.choose(self.mine, z)

        def take_outer(self):
            self.given.wait_recv()

        def take(self):
            self.come.wait_recv()
            self.choose(self.mine, z)

        def relay(self):
            self.from_rim.wait_recv()
            self.hand_on.start()

        def drain(self):
            if not (line and self.relayed):
                self.gone.wait_send()
                return

            @pl.when(outer)
            def _():
                self.to_near.wait_send()

            @pl.when(inner)
            def _():
                three = self.held.at[pl.ds(0, 3 * members)]
                to(three, three, self.send, self.send, mem=other).wait_send()

    grid = (GROUP, levels)
    row_of = lax.broadcasted_iota(jnp.int32, grid, 0)
    level_of = lax.broadcasted_iota(jnp.int32, grid, 1)
    chunk = GROUP // HALVES
    piece_level = lax.div(row_of, chunk) * lv + lax.rem(row_of, lv)
    plain = jnp.where(lax.rem(row_of, levels) == level_of, 1.0, 0.0).astype(BF16)
    pieced = jnp.where(piece_level == level_of, 1.0, 0.0).astype(BF16)
    wide = (GROUP, GROUP)
    here_of = lax.broadcasted_iota(jnp.int32, wide, 0)
    there_of = lax.div(lax.broadcasted_iota(jnp.int32, wide, 1), levels)
    same_plain = lax.div(here_of, levels) == there_of
    same_pieced = lax.div(lax.rem(here_of, chunk), lv) == there_of

    def dot(a, b):
        return jnp.dot(a, b, preferred_element_type=F32)

    def dot_nt(a, b):
        return lax.dot_general(a, b, NT, preferred_element_type=F32)

    def blocks(tall, same):
        full = dot_nt(tall.astype(BF16), plain)
        return jnp.where(same, full, 0.0).astype(BF16)

    with jax.named_scope("coef"):
        small[0].wait()
        root_terms = split(r.vroot[...])
        root = [blocks(dot(pieced, v), same_pieced) for v in root_terms]
        small[1].wait()
        small[2].wait()
        small[3].wait()

        def load(n, carry):
            for copy in loads_of(n):
                copy.start()
            return carry

        lax.fori_loop(0, units, load, 0)
        band = r.band[...].reshape(1, modes)
        gain = jnp.zeros((1, modes), F32)
        for b in range(r.band_gain.shape[0]):
            gain = jnp.where(band == b, r.band_gain[b], gain)
        r.gain[...] = gain
        for n in range(rows // GROUP):
            control = r.alpha[n * GROUP : (n + 1) * GROUP, :]
            coef = (dot(root[0], control) + dot(root[1], control)) * gain
            coef = coef.astype(BF16)
            count = GROUP // levels
            for c in range(HALVES):
                for g in range(groups):
                    block = coef[c * chunk : (c + 1) * chunk, g * gw : (g + 1) * gw]
                    at = pl.ds(z * members + n * count, count)
                    coef_held[c * groups + g][at] = block.reshape(count, lv, gw)
    with jax.named_scope("barrier"):
        pl.semaphore_wait(barrier, zn - 1 + qn)

    coef_ex = [
        Exchange(
            lambda m: r.inv_s[0, m], coef_held[p], r.coef_pack.at[p], r.pick.at[p, s], lv,
            r.z_send.at[p], r.z_recv.at[p],
        )
        for p in range(parts)
    ]
    for ex in coef_ex:
        ex.start()
    grad_ex = [
        Exchange(
            lambda m: r.order[m], grad_held[g], r.grad_pack.at[g], r.got.at[g], levels,
            r.g_send.at[g], r.g_recv.at[g], r.g_rim.at[g] if line else None,
        )
        for g in range(groups)
    ]

    small[4].wait()
    spot = lax.broadcasted_iota(jnp.int32, r.inv_v.shape, 1)
    inverse = jnp.zeros(r.inv_v.shape, jnp.int32)
    for j in range(slots):
        inverse = jnp.where(spot == r.order[j], j, inverse)
    r.inv_v[...] = inverse
    inv_copy = pltpu.make_async_copy(r.inv_v, r.inv_s, r.inv_sem)
    inv_copy.start()

    for keep, v in enumerate(root_terms):
        r.root_t[keep] = blocks(dot_nt(plain, v), same_plain)

    with jax.named_scope("weigh"):
        small[5].wait()
        small[6].wait()

        def weigh(m, carry):
            at = pl.ds(pl.multiple_of(m * levels, levels), levels)
            r.weighted[at, :] = (r.anom[m].astype(F32) * r.gradient[...].astype(F32)).astype(BF16)
            return carry

        lax.fori_loop(0, members, weigh, 0)

    def block_of(p, t):
        return r.pick.at[p, t]

    def share(p, t, recv, where):
        return to(block_of(p, t), block_of(p, t), r.pk_send.at[p], recv.at[p], state=where)

    def several(p, count, recv):
        some = r.pick.at[p, pl.ds(0, count)]
        return to(some, some, r.pk_send.at[p], recv.at[p], state=partner)

    class Gather:
        def __init__(self, p):
            there = [qpeer[k] * 2 + core for k in range(1, qn)]
            self.mate = share(p, partner, r.pk_mate, partner)
            self.gone = several(p, 2 * qn - 1, r.pk_over)
            if square:
                side = [first * 2 + core, second * 2 + core]
                self.out = [share(p, s, r.pk_side, where) for where in side]
                self.relay = share(p, side[0], r.pk_far, side[1])
                self.far = share(p, there[2], r.pk_far, partner)
                self.far_over = share(p, there[2], r.pk_last, partner)
                self.far_rest = share(p, there[2] + 1 - 2 * core, r.pk_last, partner)
            else:
                side = there
                self.out = [share(p, s, r.pk_side, where) for where in side]
            self.out.append(share(p, s, r.pk_mate, partner))
            self.side = several(p, len(side), r.pk_side)
            self.over = [share(p, t, r.pk_over, partner) for t in side]
            self.rest = several(p, len(side), r.pk_over)

        def start(self):
            for copy in self.out:
                copy.start()

        def pass_on(self):
            self.side.wait_recv()
            if square:
                self.relay.start()
            for copy in self.over:
                copy.start()

        def pass_far(self):
            if square:
                self.far.wait_recv()
                self.far_over.start()

        def finish(self):
            self.rest.wait_recv()

        def finish_far(self):
            if square:
                self.far_rest.wait_recv()

        def drain(self):
            self.gone.wait_send()

    gathers = [Gather(p) for p in range(parts)]

    def on_inner(*fns):
        def run():
            for fn in fns:
                fn()

        if line:
            pl.when(inner)(run)

    def on_outer(*fns):
        def run():
            for fn in fns:
                fn()

        if line:
            pl.when(outer)(run)

    def pair_of(n):
        return to(r.pair_out.at[n], r.pair_in.at[n], r.pair_send, r.pair_recv.at[n], state=partner)

    def scatter(g, i, dst, recv, where):
        return to(r.rs_out.at[i * groups + g], dst, r.rs_send, recv, state=where * 2 + core)

    def scatters_of(g):
        recv = r.rs_recv.at[g]
        if not square:
            return [scatter(g, i, r.rs_in.at[g * (qn - 1) + i], recv, chip_at(i, core)) for i in range(qn - 1)]
        return [
            scatter(g, 0, r.relay_in.at[g], r.relay_recv.at[g], first),
            scatter(g, 1, r.rs_in.at[g * 2], recv, first),
            scatter(g, 2, r.rs_in.at[g * 2 + 1], recv, second),
        ]

    arrivals = r.rs_in.shape[0] // groups

    def scattered(g):
        block = r.rs_in.at[pl.ds(g * arrivals, arrivals)]
        return to(block, block, r.rs_send, r.rs_recv.at[g], state=partner)

    def combine(n):
        i, g = lax.div(n, groups), lax.rem(n, groups)
        pair_of(n).wait_recv()

        @pl.when(i == qn - 1)
        def _():
            r.mine[n] = r.mine[n] + r.pair_in[n]

        copies = scatters_of(g)
        for k, copy in enumerate(copies):

            @pl.when(i == k)
            def _():
                total = r.mine[n] + r.pair_in[n]
                if square and k == 2:
                    copies[0].wait_recv()
                    total = total + r.relay_in[g].astype(F32)
                r.rs_out[n] = total.astype(BF16)
                copy.start()

    def adjoint(g):
        scattered(g).wait_recv()
        total = r.mine[(qn - 1) * groups + g]
        for i in range(arrivals):
            total = total + r.rs_in[g * arrivals + i].astype(F32)
        stack = jnp.concatenate([total[n * GROUP : (n + 1) * GROUP] for n in range(rows // GROUP)], axis=1)
        high, low = split(stack)
        grad = dot(r.root_t[0], high) + dot(r.root_t[0], low) + dot(r.root_t[1], high)
        scale = r.gain[:, g * gw : (g + 1) * gw]
        count = GROUP // levels
        for n in range(rows // GROUP):
            block = (grad[:, n * gw : (n + 1) * gw] * scale).astype(BF16)
            grad_held[g][pl.ds(z * members + n * count, count)] = block.reshape(count, levels, gw)
        grad_ex[g].start()

    inv_copy.wait()
    take_in = [ex.take_inner for ex in coef_ex] if line else []
    take_out = [ex.take_outer for ex in coef_ex] if line else []
    services = {
        3: lambda: on_inner(take_in[0], gathers[0].start),
        5: lambda: on_inner(take_in[1]),
        6: lambda: on_outer(take_out[0], gathers[0].start),
        7: lambda: on_inner(take_in[2]),
    }

    def unit(n, carry):
        i = lax.div(n, groups)
        cut = mode_rows(lax.rem(n, groups))
        loaded(n).wait()
        with jax.named_scope("unit"):
            rhs = jnp.concatenate([r.base[other_block(i), cut, :], r.base[own_block(i), cut, :]], axis=0)
            both = dot_nt(r.weighted[...], rhs)
            r.pair_out[n] = both[:, :gw]
            r.mine[n] = both[:, gw:]
        pair_of(n).start()

        @pl.when(n > 0)
        def _():
            combine(n - 1)

        if tuned:
            for at, serve in services.items():
                pl.when(n == at)(serve)
        return carry

    lax.fori_loop(0, units, unit, 0)
    if line:
        def stage_of(c, j):
            return to(r.inc_out.at[c, j], r.inc_in.at[c, j], r.inc_send.at[0], r.inc_recv.at[c, j], mem=near)

        def cross_of(c, j):
            return to(r.inc_sum.at[c, j], r.inc_got.at[c, j], r.inc_send.at[0], r.cross_recv.at[c, j], mem=other)

        def final_of(c, j, where):
            return to(r.inc_all.at[c, j], r.inc_all.at[c, j], r.inc_send.at[1], r.inc_recv.at[c, j], mem=where)

    def product(c, modes_of, at):
        lhs = [r.pick[c * groups + g, t] for g, t in modes_of]
        rhs = [r.base[t, g * gw : (g + 1) * gw, at] for g, t in modes_of]
        return dot(jnp.concatenate(lhs, axis=1), jnp.concatenate(rhs, axis=0))

    def pair_at(chips):
        return [c * 2 + side for c in chips for side in range(2)]

    home = pair_at([chip])
    sides = pair_at([first, second]) if square else pair_at([qpeer[k] for k in range(1, qn)])
    corner = pair_at([qpeer[3]]) if square else []

    def spread(c, blocks, start, last, hooks={}):
        def part(j, carry):
            for k, hook in hooks.items():
                pl.when(j == k)(hook)
            at = pl.ds(pl.multiple_of(j * width, width), width)
            field = product(c, blocks, at)
            if not start:
                field = field + r.acc[c, :, at]
            if not last:
                r.acc[c, :, at] = field
                return carry
            run = jnp.zeros((lv, width), F32)
            for m in range(members):
                run = run + field[m * lv : (m + 1) * lv] * r.anom[m, c * lv : (c + 1) * lv, at].astype(F32)
            r.inc_part[c * lv : (c + 1) * lv, at] = run
            if line:

                @pl.when(outer)
                def _():
                    r.inc_out[c, j] = run.astype(BF16)
                    stage_of(c, j).start()

            return carry

        lax.fori_loop(0, STRIPS, part, 0)

    def each(fn):
        def step(j, carry):
            fn(j)
            return carry

        lax.fori_loop(0, STRIPS, step, 0)

    def inner_sum(c):
        def one(j):
            at = pl.ds(pl.multiple_of(j * width, width), width)
            stage_of(c, j).wait_recv()
            total = r.inc_part[c * lv : (c + 1) * lv, at] + r.inc_in[c, j].astype(F32)
            r.inc_sum[c, j] = total.astype(BF16)
            cross_of(c, j).start()

        if line:
            @pl.when(inner)
            def _():
                each(one)

    def inner_final(c):
        def one(j):
            cross_of(c, j).wait_recv()
            total = r.inc_sum[c, j].astype(F32) + r.inc_got[c, j].astype(F32)
            r.inc_all[c, j] = total.astype(BF16)
            final_of(c, j, rim).start()

        if line:
            @pl.when(inner)
            def _():
                each(one)

    def grad_inner(g):
        if line and g < groups:

            @pl.when(inner)
            def _():
                grad_ex[g].take_inner()

    def scoped(name, *fns):
        with jax.named_scope(name):
            for fn in fns:
                fn()

    if tuned:
        def go(*fns):
            def run():
                for fn in fns:
                    fn()

            return run

        def of(gs, blocks):
            return [(g, t) for g in gs for t in blocks]

        scoped("start1", lambda: on_outer(take_out[1]), gathers[1].start)
        scoped("combine", lambda: combine(jnp.int32(units - 1)))
        scoped("mate", gathers[0].mate.wait_recv, gathers[1].mate.wait_recv)
        scoped("home0", lambda: spread(0, of((0, 1), home), True, False, {
            1: lambda: on_inner(take_in[3]),
            2: go(lambda: on_outer(take_out[2]), gathers[2].start),
            3: lambda: on_inner(gathers[3].start),
        }))
        scoped("adjoint0", lambda: adjoint(0))
        scoped("adjoint1", lambda: adjoint(1))
        scoped("pass0", gathers[0].pass_on)
        scoped("home1", gathers[2].mate.wait_recv, lambda: spread(1, of((0,), home), True, False))
        scoped("fin0", gathers[0].finish)
        scoped("side0", lambda: spread(0, of((0,), sides), False, False, {
            0: lambda: on_outer(take_out[3], gathers[3].start),
            1: gathers[1].pass_on,
        }))
        scoped("far0", gathers[0].pass_far)
        scoped("fin1", gathers[1].finish)
        scoped("side1", lambda: spread(0, of((1,), sides), False, False, {
            1: gathers[2].pass_on,
            2: lambda: on_inner(grad_ex[0].relay),
        }))
        scoped("home2", gathers[3].mate.wait_recv, lambda: spread(1, of((1,), home), False, False, {
            0: gathers[1].pass_far,
        }))
        scoped("finf0", gathers[0].finish_far, gathers[1].finish_far)
        scoped("corner0", lambda: spread(0, of((0, 1), corner), False, True, {
            1: gathers[3].pass_on,
            2: lambda: on_inner(grad_ex[1].relay),
            3: gathers[2].pass_far,
        }))
        scoped("fin23", gathers[2].finish, gathers[3].finish)
        scoped("side23", lambda: spread(1, of((0, 1), sides), False, False, {
            2: lambda: grad_inner(0),
            3: gathers[3].pass_far,
        }))
        scoped("finf1", gathers[2].finish_far, gathers[3].finish_far)
        scoped("corner1", lambda: spread(1, of((0, 1), corner), False, True, {1: lambda: inner_sum(0)}))
        scoped("grad1", lambda: grad_inner(1))
        scoped("sum1", lambda: inner_sum(1))
        scoped("final0", lambda: inner_final(0))
        scoped("final1", lambda: inner_final(1))
    else:
        combine(jnp.int32(units - 1))
        for p in range(parts):
            if line:
                on_inner(take_in[p])
                on_outer(take_out[p])
            else:
                coef_ex[p].take()
            gathers[p].start()
        for g in range(groups):
            adjoint(g)
        for gather in gathers:
            gather.mate.wait_recv()
            gather.pass_on()
            gather.pass_far()
        for c in range(HALVES):
            for g in range(groups):
                gathers[c * groups + g].finish()
                gathers[c * groups + g].finish_far()
                spread(c, [(g, t) for t in home + sides + corner], g == 0, g == groups - 1)
            inner_sum(c)
            inner_final(c)
        for g in range(groups):
            on_inner(grad_ex[g].relay)
            grad_inner(g)

    with jax.named_scope("settle"):
        if line:
            @pl.when(outer)
            def _():
                for ex in grad_ex:
                    ex.take_outer()
        else:
            for ex in grad_ex:
                ex.take()
        for g in range(groups):
            grad_out[:, g * gw : (g + 1) * gw] = r.got[g]

    if line:
        with jax.named_scope("last"):
            @pl.when(outer)
            def _():
                for c in range(HALVES):
                    each(lambda j, c=c: final_of(c, j, near).wait_recv())

            for c in range(HALVES):
                for j in range(STRIPS):
                    inc_out[c * lv : (c + 1) * lv, j * width : (j + 1) * width] = r.inc_all[c, j]

        to(r.inc_sum, r.inc_got, r.inc_send.at[0], r.inc_recv.at[0, 0], mem=zpeer[1]).wait_send()

        @pl.when(inner)
        def _():
            to(r.inc_all, r.inc_all, r.inc_send.at[1], r.inc_recv.at[0, 0], mem=rim).wait_send()
    else:
        strip = columns // zn
        sums = [
            to(r.inc_out.at[k], r.inc_in.at[k], r.is_send.at[k], r.is_recv.at[k], mem=zpeer[k]) for k in range(1, zn)
        ]
        for k in range(1, zn):
            at = pl.ds(pl.multiple_of(zpeer[k] * strip, strip), strip)
            r.inc_out[k] = r.inc_part[:, at].astype(BF16)
            sums[k - 1].start()
        run = r.inc_part[:, pl.ds(pl.multiple_of(z * strip, strip), strip)]
        for k in range(1, zn):
            sums[k - 1].wait_recv()
            run = run + r.inc_in[k].astype(F32)
        r.inc_all[z] = run.astype(BF16)

        def held(k, a):
            return to(r.inc_all.at[a], r.inc_all.at[a], r.if_send.at[k], r.if_recv.at[a], mem=zpeer[k])

        shares = [held(k, z) for k in range(1, zn)]
        for copy in shares:
            copy.start()
        for k in range(1, zn):
            held(k, zpeer[k]).wait_recv()
        for b in range(zn):
            inc_out[:, b * strip : (b + 1) * strip] = r.inc_all[b]
        for copy in sums + shares:
            copy.wait_send()

    with jax.named_scope("drain"):
        for ex in coef_ex + grad_ex:
            ex.drain()
        for gather in gathers:
            gather.drain()
        to(r.pair_out, r.pair_in, r.pair_send, r.pair_recv.at[0], state=partner).wait_send()
        gone = r.rs_out.at[pl.ds(0, (qn - 1) * groups)]
        to(gone, gone, r.rs_send, r.rs_recv.at[0], state=partner).wait_send()


def widen(inc, grad, inc_out, grad_out):
    inc_out[...] = inc[...].astype(F32)
    grad_out[...] = grad[...].astype(F32)


def on_device(zn, sn, anomalies, alpha, basis, gradient, vertical_root, band_gain, band, order):
    members, levels, columns = anomalies.shape
    modes = alpha.shape[2]
    rows = members * levels
    qn = sn // 2
    slots = zn * members
    gw = min(LANES, modes)
    groups = modes // gw
    lv = levels // HALVES
    parts = HALVES * groups
    arrivals = 2 if qn == 4 else qn - 1
    width = columns // STRIPS
    line = zn == 4
    vmem = pl.BlockSpec(memory_space=pltpu.VMEM)
    hbm = pl.BlockSpec(memory_space=pl.ANY)
    dma = pltpu.SemaphoreType.DMA
    lookup = (1, -(-slots // LANES) * LANES)
    scratch = dict(
        anom=pltpu.VMEM((members, levels, columns), BF16),
        base=pltpu.VMEM((sn, modes, columns), BF16),
        weighted=pltpu.VMEM((rows, columns), BF16),
        alpha=pltpu.VMEM((rows, modes), BF16),
        gradient=pltpu.VMEM((levels, columns), BF16),
        vroot=pltpu.VMEM((levels, levels), F32),
        band=pltpu.VMEM((modes,), jnp.int32),
        gain=pltpu.VMEM((1, modes), F32),
        root_t=pltpu.VMEM((2, GROUP, GROUP), BF16),
        inv_v=pltpu.VMEM(lookup, jnp.int32),
        inv_s=pltpu.SMEM(lookup, jnp.int32),
        coef_pack=pltpu.VMEM((parts, members * lv, gw), BF16),
        pick=pltpu.VMEM((parts, sn, members * lv, gw), BF16),
        pair_out=pltpu.VMEM((groups * qn, rows, gw), F32),
        pair_in=pltpu.VMEM((groups * qn, rows, gw), F32),
        mine=pltpu.VMEM((groups * qn, rows, gw), F32),
        rs_out=pltpu.VMEM((groups * qn, rows, gw), BF16),
        rs_in=pltpu.VMEM((groups * arrivals, rows, gw), BF16),
        relay_in=pltpu.VMEM((groups, rows, gw), BF16),
        grad_pack=pltpu.VMEM((groups, rows, gw), BF16),
        got=pltpu.VMEM((groups, rows, gw), BF16),
        acc=pltpu.VMEM((HALVES, members * lv, columns), F32),
        inc_part=pltpu.VMEM((levels, columns), F32),
        load_sem=dma((7,)),
        band_gain=pltpu.SMEM(band_gain.shape, F32),
        order=pltpu.SMEM(order.shape, jnp.int32),
        base_sem=dma((groups * qn,)),
        inv_sem=dma,
        z_send=dma((parts,)),
        z_recv=dma((parts,)),
        g_send=dma((groups,)),
        g_recv=dma((groups,)),
        g_rim=dma((groups,)),
        pk_send=dma((parts,)),
        pk_side=dma((parts,)),
        pk_mate=dma((parts,)),
        pk_over=dma((parts,)),
        pk_far=dma((parts,)),
        pk_last=dma((parts,)),
        pair_send=dma,
        pair_recv=dma((groups * qn,)),
        rs_send=dma,
        rs_recv=dma((groups,)),
        relay_recv=dma((groups,)),
    )
    scratch |= {f"coef_held{p}": pltpu.VMEM((slots, lv, gw), BF16) for p in range(parts)}
    scratch |= {f"grad_held{g}": pltpu.VMEM((slots, levels, gw), BF16) for g in range(groups)}
    if line:
        strips = (HALVES, STRIPS, lv, width)
        scratch |= {n: pltpu.VMEM(strips, BF16) for n in ("inc_out", "inc_in", "inc_sum", "inc_got", "inc_all")}
        scratch |= {"inc_send": dma((2,))} | {n: dma((HALVES, STRIPS)) for n in ("inc_recv", "cross_recv")}
    else:
        strips = (zn, levels, columns // zn)
        scratch |= {n: pltpu.VMEM(strips, BF16) for n in ("inc_out", "inc_in", "inc_all")}
        scratch |= {n: dma((zn,)) for n in ("is_send", "is_recv", "if_send", "if_recv")}
    increment, grads = pl.pallas_call(
        functools.partial(kernel, zn, sn, tuple(scratch)),
        out_shape=(
            jax.ShapeDtypeStruct((levels, columns), BF16),
            jax.ShapeDtypeStruct((rows, modes), BF16),
        ),
        in_specs=[hbm] * 8,
        out_specs=(vmem, vmem),
        scratch_shapes=list(scratch.values()),
        compiler_params=pltpu.CompilerParams(
            collective_id=0, has_side_effects=True, vmem_limit_bytes=58 * 2**20
        ),
    )(
        order, band_gain, vertical_root, alpha.reshape(rows, modes), band, gradient,
        anomalies, basis.reshape(sn, modes, columns),
    )
    increment, grads = pl.pallas_call(
        widen,
        out_shape=(
            jax.ShapeDtypeStruct((levels, columns), F32),
            jax.ShapeDtypeStruct((rows, modes), F32),
        ),
        in_specs=[vmem] * 2,
        out_specs=(vmem, vmem),
    )(increment, grads)
    return increment, grads.reshape(members, levels, modes)


def solution(mesh):
    zn, sn = mesh.shape["mem"], mesh.shape["state"]
    return jax.shard_map(
        functools.partial(on_device, zn, sn),
        mesh=mesh,
        in_specs=(
            P("mem", None, "state"),
            P("mem", None, "state"),
            P(None, "state"),
            P(None, "state"),
            P(),
            P(),
            P("state"),
            P(),
        ),
        out_specs=(P(None, "state"), P("mem", None, "state")),
        check_vma=False,
    )
```

```python
import functools
import types
import jax
import jax.numpy as jnp
from jax import lax
from jax.experimental import pallas as pl
from jax.experimental.pallas import tpu as pltpu
from jax.sharding import PartitionSpec as P

MESH = pl.DeviceIdType.MESH
F32 = jnp.float32
BF16 = jnp.bfloat16
NT = (((1,), (1,)), ((), ()))
LANES = 128
GROUP = 256
HALVES = 2
STRIPS = 4


def flip(a, k, n):
    out, bit, k = 0, 1, jnp.asarray(k, jnp.int32)
    while bit < n:
        out = out + lax.rem(lax.div(a, bit) + lax.div(k, bit), 2) * bit
        bit *= 2
    return out


def split(v):
    high = v.astype(BF16)
    return high, (v - high.astype(F32)).astype(BF16)


def kernel(
    zn, sn, names,
    order_h, band_gain_h, vroot_h, alpha_h, band_h, gradient_h, anomalies, basis,
    inc_out, grad_out, *scratch,
):
    r = types.SimpleNamespace(**dict(zip(names, scratch)))
    coef_held = [ref for name, ref in zip(names, scratch) if name.startswith("coef_held")]
    grad_held = [ref for name, ref in zip(names, scratch) if name.startswith("grad_held")]
    z = lax.axis_index("mem")
    s = lax.axis_index("state")
    chip, core = lax.div(s, 2), lax.rem(s, 2)
    qn = sn // 2
    partner = chip * 2 + (1 - core)
    members, levels, columns = r.anom.shape
    modes = r.alpha.shape[1]
    parts = len(coef_held)
    _, lv, gw = coef_held[0].shape
    groups = modes // gw
    rows = members * levels
    slots = zn * members
    width = columns // STRIPS
    line, square = zn == 4, qn == 4
    tuned = line and square and groups == 2

    zpeer = [flip(z, k, zn) for k in range(zn)]
    qpeer = [flip(chip, k, qn) for k in range(qn)]
    if square:
        first = qpeer[1] * (1 - core) + qpeer[2] * core
        second = qpeer[2] * (1 - core) + qpeer[1] * core

    def chip_at(i, side):
        if square:
            i = side * i + (1 - side) * (lax.rem(i, 2) * 2 + lax.div(i, 2))
        return flip(chip, qn - 1 - i, qn)

    def own_block(i):
        return chip_at(i, core) * 2 + core

    def other_block(i):
        return chip_at(i, 1 - core) * 2 + 1 - core

    small = [
        pltpu.make_async_copy(src, dst, r.load_sem.at[i])
        for i, (src, dst) in enumerate(
            [
                (vroot_h, r.vroot), (alpha_h, r.alpha), (band_h, r.band), (band_gain_h, r.band_gain),
                (order_h, r.order), (gradient_h, r.gradient), (anomalies, r.anom),
            ]
        )
    ]
    for copy in small:
        copy.start()

    barrier = pltpu.get_barrier_semaphore()
    for k in range(1, zn):
        pl.semaphore_signal(barrier, inc=1, device_id={"mem": zpeer[k]}, device_id_type=MESH)
    for k in range(1, qn):
        pl.semaphore_signal(barrier, inc=1, device_id={"state": qpeer[k] * 2 + core}, device_id_type=MESH)
    pl.semaphore_signal(barrier, inc=1, device_id={"state": partner}, device_id_type=MESH)

    def mode_rows(g):
        return pl.ds(pl.multiple_of(g * gw, gw), gw)

    def load_of(g, t, n):
        here = mode_rows(g)
        return pltpu.make_async_copy(basis.at[t, here], r.base.at[t, here], r.base_sem.at[n])

    def loaded(n):
        two = (pl.ds(0, 2), pl.ds(0, gw))
        return pltpu.make_async_copy(basis.at[two], r.base.at[two], r.base_sem.at[n])

    def loads_of(n):
        i, g = lax.div(n, groups), lax.rem(n, groups)
        return load_of(g, other_block(i), n), load_of(g, own_block(i), n)

    units = groups * qn

    def to(src, dst, send, recv, **where):
        return pltpu.make_async_remote_copy(
            src_ref=src, dst_ref=dst, send_sem=send, recv_sem=recv, device_id=where, device_id_type=MESH
        )

    own_rows = pl.ds(z * members, members)
    outer = lax.div(lax.rem(z + 1, zn), 2) == 0
    inner = jnp.logical_not(outer)
    near = 1 + lax.div(z, 2)
    mid = 3 - near
    other = 3 - z
    rim = (z - 1) * 3
    distant = 3 - rim

    class Exchange:
        def __init__(self, find, held, pack, mine, height, send, recv, rim_recv=None):
            self.find, self.held, self.pack, self.mine, self.height = find, held, pack, mine, height
            own = held.at[own_rows]
            come = held.at[pl.ds(0, (zn - 1) * members)]
            self.come = to(come, come, send, recv, mem=zpeer[1])
            gone = held.at[pl.ds(0, (2 if line else zn - 1) * members)]
            self.gone = to(gone, gone, send, recv, mem=zpeer[1])
            self.relayed, self.send = rim_recv is not None, send
            if not line:
                self.out = [to(own, own, send, recv, mem=zpeer[k]) for k in range(1, zn)]
                return
            self.to_mid = to(own, own, send, recv, mem=mid)
            self.to_near = to(own, own, send, rim_recv if self.relayed else recv, mem=near)
            self.to_other = to(own, own, send, recv, mem=other)
            if self.relayed:
                rims = held.at[pl.ds(rim * members, members)]
                self.from_rim = to(rims, rims, send, rim_recv, mem=other)
                self.hand_on = to(rims, rims, send, recv, mem=other)
                count = pl.ds(0, 2 * members)
                self.come = to(held.at[count], held.at[count], send, recv, mem=other)
            self.give = to(pack, mine, send, recv, mem=rim)
            self.given = to(pack, mine, send, recv, mem=near)

        def start(self):
            if not line:
                for copy in self.out:
                    copy.start()
                return

            @pl.when(outer)
            def _():
                if not self.relayed:
                    self.to_mid.start()
                self.to_near.start()

            @pl.when(inner)
            def _():
                self.to_other.start()

        def choose(self, out, who):
            for m in range(members):
                out[m * self.height : (m + 1) * self.height, :] = self.held[self.find(who * members + m)]

        def take_inner(self):
            self.come.wait_recv()
            self.choose(self.pack, rim)
            self.give.start()
            self.choose(self.mine, z)

        def take_outer(self):
            self.given.wait_recv()

        def take(self):
            self.come.wait_recv()
            self.choose(self.mine, z)

        def relay(self):
            self.from_rim.wait_recv()
            self.hand_on.start()

        def drain(self):
            if not (line and self.relayed):
                self.gone.wait_send()
                return

            @pl.when(outer)
            def _():
                self.to_near.wait_send()

            @pl.when(inner)
            def _():
                three = self.held.at[pl.ds(0, 3 * members)]
                to(three, three, self.send, self.send, mem=other).wait_send()

    grid = (GROUP, levels)
    row_of = lax.broadcasted_iota(jnp.int32, grid, 0)
    level_of = lax.broadcasted_iota(jnp.int32, grid, 1)
    chunk = GROUP // HALVES
    piece_level = lax.div(row_of, chunk) * lv + lax.rem(row_of, lv)
    plain = jnp.where(lax.rem(row_of, levels) == level_of, 1.0, 0.0).astype(BF16)
    pieced = jnp.where(piece_level == level_of, 1.0, 0.0).astype(BF16)
    wide = (GROUP, GROUP)
    here_of = lax.broadcasted_iota(jnp.int32, wide, 0)
    there_of = lax.div(lax.broadcasted_iota(jnp.int32, wide, 1), levels)
    same_plain = lax.div(here_of, levels) == there_of
    same_pieced = lax.div(lax.rem(here_of, chunk), lv) == there_of

    def dot(a, b):
        return jnp.dot(a, b, preferred_element_type=F32)

    def dot_nt(a, b):
        return lax.dot_general(a, b, NT, preferred_element_type=F32)

    def blocks(tall, same):
        full = dot_nt(tall.astype(BF16), plain)
        return jnp.where(same, full, 0.0).astype(BF16)

    with jax.named_scope("coef"):
        small[0].wait()
        root_terms = split(r.vroot[...])
        root = [blocks(dot(pieced, v), same_pieced) for v in root_terms]
        small[1].wait()
        small[2].wait()
        small[3].wait()

        def load(n, carry):
            for copy in loads_of(n):
                copy.start()
            return carry

        lax.fori_loop(0, units, load, 0)
        band = r.band[...].reshape(1, modes)
        gain = jnp.zeros((1, modes), F32)
        for b in range(r.band_gain.shape[0]):
            gain = jnp.where(band == b, r.band_gain[b], gain)
        r.gain[...] = gain
        for n in range(rows // GROUP):
            control = r.alpha[n * GROUP : (n + 1) * GROUP, :]
            coef = (dot(root[0], control) + dot(root[1], control)) * gain
            coef = coef.astype(BF16)
            count = GROUP // levels
            for c in range(HALVES):
                for g in range(groups):
                    block = coef[c * chunk : (c + 1) * chunk, g * gw : (g + 1) * gw]
                    at = pl.ds(z * members + n * count, count)
                    coef_held[c * groups + g][at] = block.reshape(count, lv, gw)
    with jax.named_scope("barrier"):
        pl.semaphore_wait(barrier, zn - 1 + qn)

    coef_ex = [
        Exchange(
            lambda m: r.inv_s[0, m], coef_held[p], r.coef_pack.at[p], r.pick.at[p, s], lv,
            r.z_send.at[p], r.z_recv.at[p],
        )
        for p in range(parts)
    ]
    for ex in coef_ex:
        ex.start()
    grad_ex = [
        Exchange(
            lambda m: r.order[m], grad_held[g], r.grad_pack.at[g], r.got.at[g], levels,
            r.g_send.at[g], r.g_recv.at[g], r.g_rim.at[g] if line else None,
        )
        for g in range(groups)
    ]

    small[4].wait()
    spot = lax.broadcasted_iota(jnp.int32, r.inv_v.shape, 1)
    inverse = jnp.zeros(r.inv_v.shape, jnp.int32)
    for j in range(slots):
        inverse = jnp.where(spot == r.order[j], j, inverse)
    r.inv_v[...] = inverse
    inv_copy = pltpu.make_async_copy(r.inv_v, r.inv_s, r.inv_sem)
    inv_copy.start()

    for keep, v in enumerate(root_terms):
        r.root_t[keep] = blocks(dot_nt(plain, v), same_plain)

    with jax.named_scope("weigh"):
        small[5].wait()
        small[6].wait()

        def weigh(m, carry):
            at = pl.ds(pl.multiple_of(m * levels, levels), levels)
            r.weighted[at, :] = (r.anom[m].astype(F32) * r.gradient[...].astype(F32)).astype(BF16)
            return carry

        lax.fori_loop(0, members, weigh, 0)

    def block_of(p, t):
        return r.pick.at[p, t]

    def share(p, t, recv, where):
        return to(block_of(p, t), block_of(p, t), r.pk_send.at[p], recv.at[p], state=where)

    def several(p, count, recv):
        some = r.pick.at[p, pl.ds(0, count)]
        return to(some, some, r.pk_send.at[p], recv.at[p], state=partner)

    class Gather:
        def __init__(self, p):
            there = [qpeer[k] * 2 + core for k in range(1, qn)]
            self.mate = share(p, partner, r.pk_mate, partner)
            self.gone = several(p, 2 * qn - 1, r.pk_over)
            if square:
                side = [first * 2 + core, second * 2 + core]
                self.out = [share(p, s, r.pk_side, where) for where in side]
                self.relay = share(p, side[0], r.pk_far, side[1])
                self.far = share(p, there[2], r.pk_far, partner)
                self.far_over = share(p, there[2], r.pk_last, partner)
                self.far_rest = share(p, there[2] + 1 - 2 * core, r.pk_last, partner)
            else:
                side = there
                self.out = [share(p, s, r.pk_side, where) for where in side]
            self.out.append(share(p, s, r.pk_mate, partner))
            self.side = several(p, len(side), r.pk_side)
            self.over = [share(p, t, r.pk_over, partner) for t in side]
            self.rest = several(p, len(side), r.pk_over)

        def start(self):
            for copy in self.out:
                copy.start()

        def pass_on(self):
            self.side.wait_recv()
            if square:
                self.relay.start()
            for copy in self.over:
                copy.start()

        def pass_far(self):
            if square:
                self.far.wait_recv()
                self.far_over.start()

        def finish(self):
            self.rest.wait_recv()

        def finish_far(self):
            if square:
                self.far_rest.wait_recv()

        def drain(self):
            self.gone.wait_send()

    gathers = [Gather(p) for p in range(parts)]

    def on_inner(*fns):
        def run():
            for fn in fns:
                fn()

        if line:
            pl.when(inner)(run)

    def on_outer(*fns):
        def run():
            for fn in fns:
                fn()

        if line:
            pl.when(outer)(run)

    def pair_of(n):
        return to(r.pair_out.at[n], r.pair_in.at[n], r.pair_send, r.pair_recv.at[n], state=partner)

    def scatter(g, i, dst, recv, where):
        return to(r.rs_out.at[i * groups + g], dst, r.rs_send, recv, state=where * 2 + core)

    def scatters_of(g):
        recv = r.rs_recv.at[g]
        if not square:
            return [scatter(g, i, r.rs_in.at[g * (qn - 1) + i], recv, chip_at(i, core)) for i in range(qn - 1)]
        return [
            scatter(g, 0, r.relay_in.at[g], r.relay_recv.at[g], first),
            scatter(g, 1, r.rs_in.at[g * 2], recv, first),
            scatter(g, 2, r.rs_in.at[g * 2 + 1], recv, second),
        ]

    arrivals = r.rs_in.shape[0] // groups

    def scattered(g):
        block = r.rs_in.at[pl.ds(g * arrivals, arrivals)]
        return to(block, block, r.rs_send, r.rs_recv.at[g], state=partner)

    def combine(n):
        i, g = lax.div(n, groups), lax.rem(n, groups)
        pair_of(n).wait_recv()

        @pl.when(i == qn - 1)
        def _():
            r.mine[n] = r.mine[n] + r.pair_in[n]

        copies = scatters_of(g)
        for k, copy in enumerate(copies):

            @pl.when(i == k)
            def _():
                total = r.mine[n] + r.pair_in[n]
                if square and k == 2:
                    copies[0].wait_recv()
                    total = total + r.relay_in[g].astype(F32)
                r.rs_out[n] = total.astype(BF16)
                copy.start()

    def adjoint(g):
        scattered(g).wait_recv()
        total = r.mine[(qn - 1) * groups + g]
        for i in range(arrivals):
            total = total + r.rs_in[g * arrivals + i].astype(F32)
        stack = jnp.concatenate([total[n * GROUP : (n + 1) * GROUP] for n in range(rows // GROUP)], axis=1)
        high, low = split(stack)
        grad = dot(r.root_t[0], high) + dot(r.root_t[0], low) + dot(r.root_t[1], high)
        scale = r.gain[:, g * gw : (g + 1) * gw]
        count = GROUP // levels
        for n in range(rows // GROUP):
            block = (grad[:, n * gw : (n + 1) * gw] * scale).astype(BF16)
            grad_held[g][pl.ds(z * members + n * count, count)] = block.reshape(count, levels, gw)
        grad_ex[g].start()

    inv_copy.wait()
    take_in = [ex.take_inner for ex in coef_ex] if line else []
    take_out = [ex.take_outer for ex in coef_ex] if line else []
    services = {
        3: lambda: on_inner(take_in[0]),
        5: lambda: on_inner(take_in[1]),
        6: lambda: on_outer(take_out[0], gathers[0].start),
        7: lambda: on_inner(take_in[2], gathers[0].start),
    }

    def unit(n, carry):
        i = lax.div(n, groups)
        cut = mode_rows(lax.rem(n, groups))
        loaded(n).wait()
        with jax.named_scope("unit"):
            rhs = jnp.concatenate([r.base[other_block(i), cut, :], r.base[own_block(i), cut, :]], axis=0)
            both = dot_nt(r.weighted[...], rhs)
            r.pair_out[n] = both[:, :gw]
            r.mine[n] = both[:, gw:]
        pair_of(n).start()

        @pl.when(n > 0)
        def _():
            combine(n - 1)

        if tuned:
            for at, serve in services.items():
                pl.when(n == at)(serve)
        return carry

    lax.fori_loop(0, units, unit, 0)
    if line:
        def stage_of(c, j):
            return to(r.inc_out.at[c, j], r.inc_in.at[c, j], r.inc_send.at[0], r.inc_recv.at[c, j], mem=near)

        def cross_of(c, j):
            return to(r.inc_sum.at[c, j], r.inc_got.at[c, j], r.inc_send.at[0], r.cross_recv.at[c, j], mem=other)

        def final_of(c, j, where):
            return to(r.inc_all.at[c, j], r.inc_all.at[c, j], r.inc_send.at[1], r.inc_recv.at[c, j], mem=where)

    def product(c, modes_of, at):
        lhs = [r.pick[c * groups + g, t] for g, t in modes_of]
        rhs = [r.base[t, g * gw : (g + 1) * gw, at] for g, t in modes_of]
        return dot(jnp.concatenate(lhs, axis=1), jnp.concatenate(rhs, axis=0))

    def pair_at(chips):
        return [c * 2 + side for c in chips for side in range(2)]

    home = pair_at([chip])
    sides = pair_at([first, second]) if square else pair_at([qpeer[k] for k in range(1, qn)])
    corner = pair_at([qpeer[3]]) if square else []

    def spread(c, blocks, start, last, hooks={}):
        wide = 1 if last else 2
        extent = wide * width

        def part(j, carry):
            for k, hook in hooks.items():
                pl.when(j == k // wide)(hook)
            at = pl.ds(pl.multiple_of(j * extent, extent), extent)
            field = product(c, blocks, at)
            if not start:
                field = field + r.acc[c, :, at]
            if not last:
                r.acc[c, :, at] = field
                return carry
            run = jnp.zeros((lv, width), F32)
            for m in range(members):
                run = run + field[m * lv : (m + 1) * lv] * r.anom[m, c * lv : (c + 1) * lv, at].astype(F32)
            r.inc_part[c * lv : (c + 1) * lv, at] = run
            if line:

                @pl.when(outer)
                def _():
                    r.inc_out[c, j] = run.astype(BF16)
                    stage_of(c, j).start()

            return carry

        lax.fori_loop(0, STRIPS // wide, part, 0)

    def each(fn):
        def step(j, carry):
            fn(j)
            return carry

        lax.fori_loop(0, STRIPS, step, 0)

    def inner_sum(c):
        def one(j):
            at = pl.ds(pl.multiple_of(j * width, width), width)
            stage_of(c, j).wait_recv()
            total = r.inc_part[c * lv : (c + 1) * lv, at] + r.inc_in[c, j].astype(F32)
            r.inc_sum[c, j] = total.astype(BF16)
            cross_of(c, j).start()

        if line:
            @pl.when(inner)
            def _():
                each(one)

    def inner_final(c):
        def one(j):
            cross_of(c, j).wait_recv()
            total = r.inc_sum[c, j].astype(F32) + r.inc_got[c, j].astype(F32)
            r.inc_all[c, j] = total.astype(BF16)
            final_of(c, j, rim).start()

        if line:
            @pl.when(inner)
            def _():
                each(one)

    def grad_inner(g):
        if line and g < groups:

            @pl.when(inner)
            def _():
                grad_ex[g].take_inner()

    def scoped(name, *fns):
        with jax.named_scope(name):
            for fn in fns:
                fn()

    if tuned:
        def go(*fns):
            def run():
                for fn in fns:
                    fn()

            return run

        def of(gs, blocks):
            return [(g, t) for g in gs for t in blocks]

        scoped("start1", lambda: on_outer(take_out[1]), gathers[1].start)
        scoped("combine", lambda: combine(jnp.int32(units - 1)))
        scoped("mate", gathers[0].mate.wait_recv, gathers[1].mate.wait_recv)
        scoped("home0", lambda: spread(0, of((0, 1), home), True, False, {
            1: lambda: on_inner(take_in[3], gathers[2].start),
            2: lambda: on_inner(gathers[3].start),
        }))
        scoped("adjoint0", lambda: adjoint(0))
        scoped("start2", lambda: on_outer(take_out[2], gathers[2].start))
        scoped("adjoint1", lambda: adjoint(1))
        scoped("pass0", gathers[0].pass_on)
        scoped("home1", gathers[2].mate.wait_recv, lambda: spread(1, of((0,), home), True, False, {
            2: lambda: on_outer(take_out[3], gathers[3].start),
        }))
        scoped("fin0", gathers[0].finish)
        scoped("side0", lambda: spread(0, of((0,), sides), False, False, {
            1: gathers[1].pass_on,
        }))
        scoped("fin1", gathers[1].finish)
        scoped("side1", lambda: spread(0, of((1,), sides), False, False, {
            0: gathers[0].pass_far,
            1: lambda: on_inner(grad_ex[0].relay),
            2: gathers[2].pass_on,
        }))
        scoped("home2", gathers[3].mate.wait_recv, lambda: spread(1, of((1,), home), False, False, {
            0: gathers[1].pass_far,
            2: gathers[3].pass_on,
            3: lambda: on_inner(grad_ex[1].relay),
        }))
        scoped("finf0", gathers[0].finish_far, gathers[1].finish_far)
        scoped("corner0", lambda: spread(0, of((0, 1), corner), False, True, {
            1: gathers[2].pass_far,
            3: gathers[3].pass_far,
        }))
        scoped("fin23", gathers[2].finish, gathers[3].finish)
        scoped("side23", lambda: spread(1, of((0, 1), sides), False, False, {
            1: lambda: grad_inner(0),
            3: lambda: inner_sum(0),
        }))
        scoped("finf1", gathers[2].finish_far, gathers[3].finish_far)
        scoped("corner1", lambda: spread(1, of((0, 1), corner), False, True, {0: lambda: grad_inner(1)}))
        scoped("sum1", lambda: inner_sum(1))
        scoped("final0", lambda: inner_final(0))
        scoped("final1", lambda: inner_final(1))
    else:
        combine(jnp.int32(units - 1))
        for p in range(parts):
            if line:
                on_inner(take_in[p])
                on_outer(take_out[p])
            else:
                coef_ex[p].take()
            gathers[p].start()
        for g in range(groups):
            adjoint(g)
        for gather in gathers:
            gather.mate.wait_recv()
            gather.pass_on()
            gather.pass_far()
        for c in range(HALVES):
            for g in range(groups):
                gathers[c * groups + g].finish()
                gathers[c * groups + g].finish_far()
                spread(c, [(g, t) for t in home + sides + corner], g == 0, g == groups - 1)
            inner_sum(c)
            inner_final(c)
        for g in range(groups):
            on_inner(grad_ex[g].relay)
            grad_inner(g)

    with jax.named_scope("settle"):
        if line:
            @pl.when(outer)
            def _():
                for ex in grad_ex:
                    ex.take_outer()
        else:
            for ex in grad_ex:
                ex.take()
        for g in range(groups):
            grad_out[:, g * gw : (g + 1) * gw] = r.got[g]

    if line:
        with jax.named_scope("last"):
            @pl.when(outer)
            def _():
                for c in range(HALVES):
                    each(lambda j, c=c: final_of(c, j, near).wait_recv())

            for c in range(HALVES):
                for j in range(STRIPS):
                    inc_out[c * lv : (c + 1) * lv, j * width : (j + 1) * width] = r.inc_all[c, j]

        to(r.inc_sum, r.inc_got, r.inc_send.at[0], r.inc_recv.at[0, 0], mem=zpeer[1]).wait_send()

        @pl.when(inner)
        def _():
            to(r.inc_all, r.inc_all, r.inc_send.at[1], r.inc_recv.at[0, 0], mem=rim).wait_send()
    else:
        strip = columns // zn
        sums = [
            to(r.inc_out.at[k], r.inc_in.at[k], r.is_send.at[k], r.is_recv.at[k], mem=zpeer[k]) for k in range(1, zn)
        ]
        for k in range(1, zn):
            at = pl.ds(pl.multiple_of(zpeer[k] * strip, strip), strip)
            r.inc_out[k] = r.inc_part[:, at].astype(BF16)
            sums[k - 1].start()
        run = r.inc_part[:, pl.ds(pl.multiple_of(z * strip, strip), strip)]
        for k in range(1, zn):
            sums[k - 1].wait_recv()
            run = run + r.inc_in[k].astype(F32)
        r.inc_all[z] = run.astype(BF16)

        def held(k, a):
            return to(r.inc_all.at[a], r.inc_all.at[a], r.if_send.at[k], r.if_recv.at[a], mem=zpeer[k])

        shares = [held(k, z) for k in range(1, zn)]
        for copy in shares:
            copy.start()
        for k in range(1, zn):
            held(k, zpeer[k]).wait_recv()
        for b in range(zn):
            inc_out[:, b * strip : (b + 1) * strip] = r.inc_all[b]
        for copy in sums + shares:
            copy.wait_send()

    with jax.named_scope("drain"):
        for ex in coef_ex + grad_ex:
            ex.drain()
        for gather in gathers:
            gather.drain()
        to(r.pair_out, r.pair_in, r.pair_send, r.pair_recv.at[0], state=partner).wait_send()
        gone = r.rs_out.at[pl.ds(0, (qn - 1) * groups)]
        to(gone, gone, r.rs_send, r.rs_recv.at[0], state=partner).wait_send()


def widen(inc, grad, inc_out, grad_out):
    inc_out[...] = inc[...].astype(F32)
    grad_out[...] = grad[...].astype(F32)


def on_device(zn, sn, anomalies, alpha, basis, gradient, vertical_root, band_gain, band, order):
    members, levels, columns = anomalies.shape
    modes = alpha.shape[2]
    rows = members * levels
    qn = sn // 2
    slots = zn * members
    gw = min(LANES, modes)
    groups = modes // gw
    lv = levels // HALVES
    parts = HALVES * groups
    arrivals = 2 if qn == 4 else qn - 1
    width = columns // STRIPS
    line = zn == 4
    vmem = pl.BlockSpec(memory_space=pltpu.VMEM)
    hbm = pl.BlockSpec(memory_space=pl.ANY)
    dma = pltpu.SemaphoreType.DMA
    lookup = (1, -(-slots // LANES) * LANES)
    scratch = dict(
        anom=pltpu.VMEM((members, levels, columns), BF16),
        base=pltpu.VMEM((sn, modes, columns), BF16),
        weighted=pltpu.VMEM((rows, columns), BF16),
        alpha=pltpu.VMEM((rows, modes), BF16),
        gradient=pltpu.VMEM((levels, columns), BF16),
        vroot=pltpu.VMEM((levels, levels), F32),
        band=pltpu.VMEM((modes,), jnp.int32),
        gain=pltpu.VMEM((1, modes), F32),
        root_t=pltpu.VMEM((2, GROUP, GROUP), BF16),
        inv_v=pltpu.VMEM(lookup, jnp.int32),
        inv_s=pltpu.SMEM(lookup, jnp.int32),
        coef_pack=pltpu.VMEM((parts, members * lv, gw), BF16),
        pick=pltpu.VMEM((parts, sn, members * lv, gw), BF16),
        pair_out=pltpu.VMEM((groups * qn, rows, gw), F32),
        pair_in=pltpu.VMEM((groups * qn, rows, gw), F32),
        mine=pltpu.VMEM((groups * qn, rows, gw), F32),
        rs_out=pltpu.VMEM((groups * qn, rows, gw), BF16),
        rs_in=pltpu.VMEM((groups * arrivals, rows, gw), BF16),
        relay_in=pltpu.VMEM((groups, rows, gw), BF16),
        grad_pack=pltpu.VMEM((groups, rows, gw), BF16),
        got=pltpu.VMEM((groups, rows, gw), BF16),
        acc=pltpu.VMEM((HALVES, members * lv, columns), F32),
        inc_part=pltpu.VMEM((levels, columns), F32),
        load_sem=dma((7,)),
        band_gain=pltpu.SMEM(band_gain.shape, F32),
        order=pltpu.SMEM(order.shape, jnp.int32),
        base_sem=dma((groups * qn,)),
        inv_sem=dma,
        z_send=dma((parts,)),
        z_recv=dma((parts,)),
        g_send=dma((groups,)),
        g_recv=dma((groups,)),
        g_rim=dma((groups,)),
        pk_send=dma((parts,)),
        pk_side=dma((parts,)),
        pk_mate=dma((parts,)),
        pk_over=dma((parts,)),
        pk_far=dma((parts,)),
        pk_last=dma((parts,)),
        pair_send=dma,
        pair_recv=dma((groups * qn,)),
        rs_send=dma,
        rs_recv=dma((groups,)),
        relay_recv=dma((groups,)),
    )
    scratch |= {f"coef_held{p}": pltpu.VMEM((slots, lv, gw), BF16) for p in range(parts)}
    scratch |= {f"grad_held{g}": pltpu.VMEM((slots, levels, gw), BF16) for g in range(groups)}
    if line:
        strips = (HALVES, STRIPS, lv, width)
        scratch |= {n: pltpu.VMEM(strips, BF16) for n in ("inc_out", "inc_in", "inc_sum", "inc_got", "inc_all")}
        scratch |= {"inc_send": dma((2,))} | {n: dma((HALVES, STRIPS)) for n in ("inc_recv", "cross_recv")}
    else:
        strips = (zn, levels, columns // zn)
        scratch |= {n: pltpu.VMEM(strips, BF16) for n in ("inc_out", "inc_in", "inc_all")}
        scratch |= {n: dma((zn,)) for n in ("is_send", "is_recv", "if_send", "if_recv")}
    increment, grads = pl.pallas_call(
        functools.partial(kernel, zn, sn, tuple(scratch)),
        out_shape=(
            jax.ShapeDtypeStruct((levels, columns), BF16),
            jax.ShapeDtypeStruct((rows, modes), BF16),
        ),
        in_specs=[hbm] * 8,
        out_specs=(vmem, vmem),
        scratch_shapes=list(scratch.values()),
        compiler_params=pltpu.CompilerParams(
            collective_id=0, has_side_effects=True, vmem_limit_bytes=58 * 2**20
        ),
    )(
        order, band_gain, vertical_root, alpha.reshape(rows, modes), band, gradient,
        anomalies, basis.reshape(sn, modes, columns),
    )
    increment, grads = pl.pallas_call(
        widen,
        out_shape=(
            jax.ShapeDtypeStruct((levels, columns), F32),
            jax.ShapeDtypeStruct((rows, modes), F32),
        ),
        in_specs=[vmem] * 2,
        out_specs=(vmem, vmem),
    )(increment, grads)
    return increment, grads.reshape(members, levels, modes)


def solution(mesh):
    zn, sn = mesh.shape["mem"], mesh.shape["state"]
    return jax.shard_map(
        functools.partial(on_device, zn, sn),
        mesh=mesh,
        in_specs=(
            P("mem", None, "state"),
            P("mem", None, "state"),
            P(None, "state"),
            P(None, "state"),
            P(),
            P(),
            P("state"),
            P(),
        ),
        out_specs=(P(None, "state"), P("mem", None, "state")),
        check_vma=False,
    )
```

```python
import functools
import types
import jax
import jax.numpy as jnp
from jax import lax
from jax.experimental import pallas as pl
from jax.experimental.pallas import tpu as pltpu
from jax.sharding import PartitionSpec as P

MESH = pl.DeviceIdType.MESH
F32 = jnp.float32
BF16 = jnp.bfloat16
NT = (((1,), (1,)), ((), ()))
LANES = 128
GROUP = 256
HALVES = 2
STRIPS = 4


def flip(a, k, n):
    out, bit, k = 0, 1, jnp.asarray(k, jnp.int32)
    while bit < n:
        out = out + lax.rem(lax.div(a, bit) + lax.div(k, bit), 2) * bit
        bit *= 2
    return out


def split(v):
    high = v.astype(BF16)
    return high, (v - high.astype(F32)).astype(BF16)


def kernel(
    zn, sn, names,
    order_h, band_gain_h, vroot_h, alpha_h, band_h, gradient_h, anomalies, basis,
    inc_out, grad_out, *scratch,
):
    r = types.SimpleNamespace(**dict(zip(names, scratch)))
    coef_held = [ref for name, ref in zip(names, scratch) if name.startswith("coef_held")]
    grad_held = [ref for name, ref in zip(names, scratch) if name.startswith("grad_held")]
    z = lax.axis_index("mem")
    s = lax.axis_index("state")
    chip, core = lax.div(s, 2), lax.rem(s, 2)
    qn = sn // 2
    partner = chip * 2 + (1 - core)
    members, levels, columns = r.anom.shape
    modes = r.alpha.shape[1]
    parts = len(coef_held)
    _, lv, gw = coef_held[0].shape
    groups = modes // gw
    rows = members * levels
    slots = zn * members
    width = columns // STRIPS
    line, square = zn == 4, qn == 4
    tuned = line and square and groups == 2

    zpeer = [flip(z, k, zn) for k in range(zn)]
    qpeer = [flip(chip, k, qn) for k in range(qn)]
    if square:
        first = qpeer[1] * (1 - core) + qpeer[2] * core
        second = qpeer[2] * (1 - core) + qpeer[1] * core

    def chip_at(i, side):
        if square:
            i = side * i + (1 - side) * (lax.rem(i, 2) * 2 + lax.div(i, 2))
        return flip(chip, qn - 1 - i, qn)

    def own_block(i):
        return chip_at(i, core) * 2 + core

    def other_block(i):
        return chip_at(i, 1 - core) * 2 + 1 - core

    small = [
        pltpu.make_async_copy(src, dst, r.load_sem.at[i])
        for i, (src, dst) in enumerate(
            [
                (vroot_h, r.vroot), (alpha_h, r.alpha), (band_h, r.band), (band_gain_h, r.band_gain),
                (order_h, r.order), (gradient_h, r.gradient), (anomalies, r.anom),
            ]
        )
    ]
    for copy in small:
        copy.start()

    barrier = pltpu.get_barrier_semaphore()
    for k in range(1, zn):
        pl.semaphore_signal(barrier, inc=1, device_id={"mem": zpeer[k]}, device_id_type=MESH)
    for k in range(1, qn):
        pl.semaphore_signal(barrier, inc=1, device_id={"state": qpeer[k] * 2 + core}, device_id_type=MESH)
    pl.semaphore_signal(barrier, inc=1, device_id={"state": partner}, device_id_type=MESH)

    def mode_rows(g):
        return pl.ds(pl.multiple_of(g * gw, gw), gw)

    def load_of(g, t, n):
        here = mode_rows(g)
        return pltpu.make_async_copy(basis.at[t, here], r.base.at[t, here], r.base_sem.at[n])

    def loaded(n):
        two = (pl.ds(0, 2), pl.ds(0, gw))
        return pltpu.make_async_copy(basis.at[two], r.base.at[two], r.base_sem.at[n])

    def loads_of(n):
        i, g = lax.div(n, groups), lax.rem(n, groups)
        return load_of(g, other_block(i), n), load_of(g, own_block(i), n)

    units = groups * qn

    def to(src, dst, send, recv, **where):
        return pltpu.make_async_remote_copy(
            src_ref=src, dst_ref=dst, send_sem=send, recv_sem=recv, device_id=where, device_id_type=MESH
        )

    own_rows = pl.ds(z * members, members)
    outer = lax.div(lax.rem(z + 1, zn), 2) == 0
    inner = jnp.logical_not(outer)
    near = 1 + lax.div(z, 2)
    mid = 3 - near
    other = 3 - z
    rim = (z - 1) * 3
    distant = 3 - rim

    class Exchange:
        def __init__(self, find, held, pack, mine, height, send, recv, rim_recv=None):
            self.find, self.held, self.pack, self.mine, self.height = find, held, pack, mine, height
            own = held.at[own_rows]
            come = held.at[pl.ds(0, (zn - 1) * members)]
            self.come = to(come, come, send, recv, mem=zpeer[1])
            gone = held.at[pl.ds(0, (2 if line else zn - 1) * members)]
            self.gone = to(gone, gone, send, recv, mem=zpeer[1])
            self.relayed, self.send = rim_recv is not None, send
            if not line:
                self.out = [to(own, own, send, recv, mem=zpeer[k]) for k in range(1, zn)]
                return
            self.to_mid = to(own, own, send, recv, mem=mid)
            self.to_near = to(own, own, send, rim_recv if self.relayed else recv, mem=near)
            self.to_other = to(own, own, send, recv, mem=other)
            if self.relayed:
                rims = held.at[pl.ds(rim * members, members)]
                self.from_rim = to(rims, rims, send, rim_recv, mem=other)
                self.hand_on = to(rims, rims, send, recv, mem=other)
                count = pl.ds(0, 2 * members)
                self.come = to(held.at[count], held.at[count], send, recv, mem=other)
            self.give = to(pack, mine, send, recv, mem=rim)
            self.given = to(pack, mine, send, recv, mem=near)

        def start(self):
            if not line:
                for copy in self.out:
                    copy.start()
                return

            @pl.when(outer)
            def _():
                if not self.relayed:
                    self.to_mid.start()
                self.to_near.start()

            @pl.when(inner)
            def _():
                self.to_other.start()

        def choose(self, out, who):
            for m in range(members):
                out[m * self.height : (m + 1) * self.height, :] = self.held[self.find(who * members + m)]

        def take_inner(self):
            self.come.wait_recv()
            self.choose(self.pack, rim)
            self.give.start()
            self.choose(self.mine, z)

        def take_outer(self):
            self.given.wait_recv()

        def take(self):
            self.come.wait_recv()
            self.choose(self.mine, z)

        def relay(self):
            self.from_rim.wait_recv()
            self.hand_on.start()

        def drain(self):
            if not (line and self.relayed):
                self.gone.wait_send()
                return

            @pl.when(outer)
            def _():
                self.to_near.wait_send()

            @pl.when(inner)
            def _():
                three = self.held.at[pl.ds(0, 3 * members)]
                to(three, three, self.send, self.send, mem=other).wait_send()

    grid = (GROUP, levels)
    row_of = lax.broadcasted_iota(jnp.int32, grid, 0)
    level_of = lax.broadcasted_iota(jnp.int32, grid, 1)
    chunk = GROUP // HALVES
    piece_level = lax.div(row_of, chunk) * lv + lax.rem(row_of, lv)
    plain = jnp.where(lax.rem(row_of, levels) == level_of, 1.0, 0.0).astype(BF16)
    pieced = jnp.where(piece_level == level_of, 1.0, 0.0).astype(BF16)
    wide = (GROUP, GROUP)
    here_of = lax.broadcasted_iota(jnp.int32, wide, 0)
    there_of = lax.div(lax.broadcasted_iota(jnp.int32, wide, 1), levels)
    same_plain = lax.div(here_of, levels) == there_of
    same_pieced = lax.div(lax.rem(here_of, chunk), lv) == there_of

    def dot(a, b):
        return jnp.dot(a, b, preferred_element_type=F32)

    def dot_nt(a, b):
        return lax.dot_general(a, b, NT, preferred_element_type=F32)

    def blocks(tall, same):
        full = dot_nt(tall.astype(BF16), plain)
        return jnp.where(same, full, 0.0).astype(BF16)

    with jax.named_scope("coef"):
        small[0].wait()
        root_terms = split(r.vroot[...])
        root = [blocks(dot(pieced, v), same_pieced) for v in root_terms]
        small[1].wait()
        small[2].wait()
        small[3].wait()

        def load(n, carry):
            for copy in loads_of(n):
                copy.start()
            return carry

        lax.fori_loop(0, units, load, 0)
        band = r.band[...].reshape(1, modes)
        gain = jnp.zeros((1, modes), F32)
        for b in range(r.band_gain.shape[0]):
            gain = jnp.where(band == b, r.band_gain[b], gain)
        r.gain[...] = gain
        for n in range(rows // GROUP):
            control = r.alpha[n * GROUP : (n + 1) * GROUP, :]
            coef = (dot(root[0], control) + dot(root[1], control)) * gain
            coef = coef.astype(BF16)
            count = GROUP // levels
            for c in range(HALVES):
                for g in range(groups):
                    block = coef[c * chunk : (c + 1) * chunk, g * gw : (g + 1) * gw]
                    at = pl.ds(z * members + n * count, count)
                    coef_held[c * groups + g][at] = block.reshape(count, lv, gw)
    with jax.named_scope("barrier"):
        pl.semaphore_wait(barrier, zn - 1 + qn)

    coef_ex = [
        Exchange(
            lambda m: r.inv_s[0, m], coef_held[p], r.coef_pack.at[p], r.pick.at[p, s], lv,
            r.z_send.at[p], r.z_recv.at[p],
        )
        for p in range(parts)
    ]
    for ex in coef_ex:
        ex.start()
    grad_ex = [
        Exchange(
            lambda m: r.order[m], grad_held[g], r.grad_pack.at[g], r.got.at[g], levels,
            r.g_send.at[g], r.g_recv.at[g], r.g_rim.at[g] if line else None,
        )
        for g in range(groups)
    ]

    small[4].wait()
    spot = lax.broadcasted_iota(jnp.int32, r.inv_v.shape, 1)
    inverse = jnp.zeros(r.inv_v.shape, jnp.int32)
    for j in range(slots):
        inverse = jnp.where(spot == r.order[j], j, inverse)
    r.inv_v[...] = inverse
    inv_copy = pltpu.make_async_copy(r.inv_v, r.inv_s, r.inv_sem)
    inv_copy.start()

    for keep, v in enumerate(root_terms):
        r.root_t[keep] = blocks(dot_nt(plain, v), same_plain)

    with jax.named_scope("weigh"):
        small[5].wait()
        small[6].wait()

        def weigh(m, carry):
            at = pl.ds(pl.multiple_of(m * levels, levels), levels)
            r.weighted[at, :] = (r.anom[m].astype(F32) * r.gradient[...].astype(F32)).astype(BF16)
            return carry

        lax.fori_loop(0, members, weigh, 0)

    def block_of(p, t):
        return r.pick.at[p, t]

    def share(p, t, recv, where):
        return to(block_of(p, t), block_of(p, t), r.pk_send.at[p], recv.at[p], state=where)

    def several(p, count, recv):
        some = r.pick.at[p, pl.ds(0, count)]
        return to(some, some, r.pk_send.at[p], recv.at[p], state=partner)

    class Gather:
        def __init__(self, p):
            there = [qpeer[k] * 2 + core for k in range(1, qn)]
            self.mate = share(p, partner, r.pk_mate, partner)
            self.gone = several(p, 2 * qn - 1, r.pk_over)
            if square:
                side = [first * 2 + core, second * 2 + core]
                self.out = [share(p, s, r.pk_side, where) for where in side]
                self.relay = share(p, side[0], r.pk_far, side[1])
                self.far = share(p, there[2], r.pk_far, partner)
                self.far_over = share(p, there[2], r.pk_last, partner)
                self.far_rest = share(p, there[2] + 1 - 2 * core, r.pk_last, partner)
            else:
                side = there
                self.out = [share(p, s, r.pk_side, where) for where in side]
            self.out.append(share(p, s, r.pk_mate, partner))
            self.side = several(p, len(side), r.pk_side)
            self.over = [share(p, t, r.pk_over, partner) for t in side]
            self.rest = several(p, len(side), r.pk_over)

        def start(self):
            for copy in self.out:
                copy.start()

        def pass_on(self):
            self.side.wait_recv()
            if square:
                self.relay.start()
            for copy in self.over:
                copy.start()

        def pass_far(self):
            if square:
                self.far.wait_recv()
                self.far_over.start()

        def finish(self):
            self.rest.wait_recv()

        def finish_far(self):
            if square:
                self.far_rest.wait_recv()

        def drain(self):
            self.gone.wait_send()

    gathers = [Gather(p) for p in range(parts)]

    def on_inner(*fns):
        def run():
            for fn in fns:
                fn()

        if line:
            pl.when(inner)(run)

    def on_outer(*fns):
        def run():
            for fn in fns:
                fn()

        if line:
            pl.when(outer)(run)

    def pair_of(n):
        return to(r.pair_out.at[n], r.pair_in.at[n], r.pair_send, r.pair_recv.at[n], state=partner)

    def scatter(g, i, dst, recv, where):
        return to(r.rs_out.at[i * groups + g], dst, r.rs_send, recv, state=where * 2 + core)

    def scatters_of(g):
        recv = r.rs_recv.at[g]
        if not square:
            return [scatter(g, i, r.rs_in.at[g * (qn - 1) + i], recv, chip_at(i, core)) for i in range(qn - 1)]
        return [
            scatter(g, 0, r.relay_in.at[g], r.relay_recv.at[g], first),
            scatter(g, 1, r.rs_in.at[g * 2], recv, first),
            scatter(g, 2, r.rs_in.at[g * 2 + 1], recv, second),
        ]

    arrivals = r.rs_in.shape[0] // groups

    def scattered(g):
        block = r.rs_in.at[pl.ds(g * arrivals, arrivals)]
        return to(block, block, r.rs_send, r.rs_recv.at[g], state=partner)

    def combine(n):
        i, g = lax.div(n, groups), lax.rem(n, groups)
        pair_of(n).wait_recv()

        @pl.when(i == qn - 1)
        def _():
            r.mine[n] = r.mine[n] + r.pair_in[n]

        copies = scatters_of(g)
        for k, copy in enumerate(copies):

            @pl.when(i == k)
            def _():
                total = r.mine[n] + r.pair_in[n]
                if square and k == 2:
                    copies[0].wait_recv()
                    total = total + r.relay_in[g].astype(F32)
                r.rs_out[n] = total.astype(BF16)
                copy.start()

    def adjoint(g):
        scattered(g).wait_recv()
        total = r.mine[(qn - 1) * groups + g]
        for i in range(arrivals):
            total = total + r.rs_in[g * arrivals + i].astype(F32)
        stack = jnp.concatenate([total[n * GROUP : (n + 1) * GROUP] for n in range(rows // GROUP)], axis=1)
        high, low = split(stack)
        grad = dot(r.root_t[0], high) + dot(r.root_t[0], low) + dot(r.root_t[1], high)
        scale = r.gain[:, g * gw : (g + 1) * gw]
        count = GROUP // levels
        for n in range(rows // GROUP):
            block = (grad[:, n * gw : (n + 1) * gw] * scale).astype(BF16)
            grad_held[g][pl.ds(z * members + n * count, count)] = block.reshape(count, levels, gw)
        grad_ex[g].start()

    inv_copy.wait()
    take_in = [ex.take_inner for ex in coef_ex] if line else []
    take_out = [ex.take_outer for ex in coef_ex] if line else []
    services = {
        3: lambda: on_inner(take_in[0]),
        5: lambda: on_inner(take_in[1]),
        6: lambda: on_outer(take_out[0], gathers[0].start),
        7: lambda: on_inner(take_in[2], gathers[0].start),
    }

    def unit(n, carry):
        i = lax.div(n, groups)
        cut = mode_rows(lax.rem(n, groups))
        loaded(n).wait()
        with jax.named_scope("unit"):
            rhs = jnp.concatenate([r.base[other_block(i), cut, :], r.base[own_block(i), cut, :]], axis=0)
            both = dot_nt(r.weighted[...], rhs)
            r.pair_out[n] = both[:, :gw]
            r.mine[n] = both[:, gw:]
        pair_of(n).start()

        @pl.when(n > 0)
        def _():
            combine(n - 1)

        if tuned:
            for at, serve in services.items():
                pl.when(n == at)(serve)
        return carry

    lax.fori_loop(0, units, unit, 0)
    if line:
        def stage_of(c, j):
            return to(r.inc_out.at[c, j], r.inc_in.at[c, j], r.inc_send.at[0], r.inc_recv.at[c, j], mem=near)

        def cross_of(c, j):
            return to(r.inc_sum.at[c, j], r.inc_got.at[c, j], r.inc_send.at[0], r.cross_recv.at[c, j], mem=other)

        def final_of(c, j, where):
            return to(r.inc_all.at[c, j], r.inc_all.at[c, j], r.inc_send.at[1], r.inc_recv.at[c, j], mem=where)

    def product(c, modes_of, at):
        lhs = [r.pick[c * groups + g, t] for g, t in modes_of]
        rhs = [r.base[t, g * gw : (g + 1) * gw, at] for g, t in modes_of]
        return dot(jnp.concatenate(lhs, axis=1), jnp.concatenate(rhs, axis=0))

    def pair_at(chips):
        return [c * 2 + side for c in chips for side in range(2)]

    home = pair_at([chip])
    sides = pair_at([first, second]) if square else pair_at([qpeer[k] for k in range(1, qn)])
    corner = pair_at([qpeer[3]]) if square else []

    def spread(c, blocks, start, last, hooks={}):
        wide = 1 if last else 2
        extent = wide * width

        def part(j, carry):
            for k, hook in hooks.items():
                pl.when(j == k // wide)(hook)
            at = pl.ds(pl.multiple_of(j * extent, extent), extent)
            field = product(c, blocks, at)
            if not start:
                field = field + r.acc[c, :, at]
            if not last:
                r.acc[c, :, at] = field
                return carry
            run = jnp.zeros((lv, width), F32)
            for m in range(members):
                run = run + field[m * lv : (m + 1) * lv] * r.anom[m, c * lv : (c + 1) * lv, at].astype(F32)
            r.inc_part[c * lv : (c + 1) * lv, at] = run
            if line:

                @pl.when(outer)
                def _():
                    r.inc_out[c, j] = run.astype(BF16)
                    stage_of(c, j).start()

            return carry

        lax.fori_loop(0, STRIPS // wide, part, 0)

    def each(fn):
        def step(j, carry):
            fn(j)
            return carry

        lax.fori_loop(0, STRIPS, step, 0)

    def inner_sum(c):
        def one(j):
            at = pl.ds(pl.multiple_of(j * width, width), width)
            stage_of(c, j).wait_recv()
            total = r.inc_part[c * lv : (c + 1) * lv, at] + r.inc_in[c, j].astype(F32)
            r.inc_sum[c, j] = total.astype(BF16)
            cross_of(c, j).start()

        if line:
            @pl.when(inner)
            def _():
                each(one)

    def inner_final(c):
        def one(j):
            cross_of(c, j).wait_recv()
            total = r.inc_sum[c, j].astype(F32) + r.inc_got[c, j].astype(F32)
            r.inc_all[c, j] = total.astype(BF16)
            final_of(c, j, rim).start()

        if line:
            @pl.when(inner)
            def _():
                each(one)

    def grad_inner(g):
        if line and g < groups:

            @pl.when(inner)
            def _():
                grad_ex[g].take_inner()

    def scoped(name, *fns):
        with jax.named_scope(name):
            for fn in fns:
                fn()

    if tuned:
        def go(*fns):
            def run():
                for fn in fns:
                    fn()

            return run

        def of(gs, blocks):
            return [(g, t) for g in gs for t in blocks]

        scoped("start1", lambda: on_outer(take_out[1]), gathers[1].start)
        scoped("combine", lambda: combine(jnp.int32(units - 1)))
        scoped("mate", gathers[0].mate.wait_recv, gathers[1].mate.wait_recv)
        scoped("home0", lambda: spread(0, of((0, 1), home), True, False, {
            1: lambda: on_inner(take_in[3]),
        }))
        scoped("adjoint0", lambda: adjoint(0))
        scoped("start2", lambda: on_outer(take_out[2]), gathers[2].start)
        scoped("adjoint1", lambda: adjoint(1))
        scoped("pass0", gathers[0].pass_on)
        scoped("home1", gathers[2].mate.wait_recv, lambda: spread(1, of((0,), home), True, False, {
            2: go(lambda: on_outer(take_out[3]), gathers[3].start),
        }))
        scoped("fin0", gathers[0].finish)
        scoped("side0", lambda: spread(0, of((0,), sides), False, False, {
            1: gathers[1].pass_on,
        }))
        scoped("fin1", gathers[1].finish)
        scoped("side1", lambda: spread(0, of((1,), sides), False, False, {0: gathers[0].pass_far, 2: go(gathers[2].pass_on, lambda: on_inner(grad_ex[0].relay))}))
        scoped("home2", gathers[3].mate.wait_recv, lambda: spread(1, of((1,), home), False, False, {0: gathers[1].pass_far, 2: gathers[3].pass_on}))
        scoped("finf0", gathers[0].finish_far, gathers[1].finish_far)
        scoped("corner0", lambda: spread(0, of((0, 1), corner), False, True, {0: lambda: on_inner(grad_ex[1].relay), 3: gathers[2].pass_far}))
        scoped("fin23", gathers[2].finish, gathers[3].finish)
        scoped("side23", lambda: spread(1, of((0, 1), sides), False, False, {0: lambda: grad_inner(0), 2: go(gathers[3].pass_far, lambda: inner_sum(0))}))
        scoped("finf1", gathers[2].finish_far, gathers[3].finish_far)
        scoped("corner1", lambda: spread(1, of((0, 1), corner), False, True, {0: lambda: grad_inner(1)}))
        scoped("sum1", lambda: inner_sum(1))
        scoped("final0", lambda: inner_final(0))
        scoped("final1", lambda: inner_final(1))
    else:
        combine(jnp.int32(units - 1))
        for p in range(parts):
            if line:
                on_inner(take_in[p])
                on_outer(take_out[p])
            else:
                coef_ex[p].take()
            gathers[p].start()
        for g in range(groups):
            adjoint(g)
        for gather in gathers:
            gather.mate.wait_recv()
            gather.pass_on()
            gather.pass_far()
        for c in range(HALVES):
            for g in range(groups):
                gathers[c * groups + g].finish()
                gathers[c * groups + g].finish_far()
                spread(c, [(g, t) for t in home + sides + corner], g == 0, g == groups - 1)
            inner_sum(c)
            inner_final(c)
        for g in range(groups):
            on_inner(grad_ex[g].relay)
            grad_inner(g)

    with jax.named_scope("settle"):
        if line:
            @pl.when(outer)
            def _():
                for ex in grad_ex:
                    ex.take_outer()
        else:
            for ex in grad_ex:
                ex.take()
        leaving = [
            pltpu.make_async_copy(r.got.at[g], grad_out.at[:, pl.ds(g * gw, gw)], r.out_sem.at[g]) for g in range(groups)
        ]
        for copy in leaving:
            copy.start()

    if line:
        with jax.named_scope("last"):
            for c in range(HALVES):

                @pl.when(outer)
                def _():
                    each(lambda j, c=c: final_of(c, j, near).wait_recv())

                for j in range(STRIPS):
                    at = (pl.ds(c * lv, lv), pl.ds(j * width, width))
                    leaving.append(
                        pltpu.make_async_copy(r.inc_all.at[c, j], inc_out.at[at], r.out_sem.at[groups + c * STRIPS + j])
                    )
                    leaving[-1].start()

        to(r.inc_sum, r.inc_got, r.inc_send.at[0], r.inc_recv.at[0, 0], mem=zpeer[1]).wait_send()

        @pl.when(inner)
        def _():
            to(r.inc_all, r.inc_all, r.inc_send.at[1], r.inc_recv.at[0, 0], mem=rim).wait_send()
    else:
        strip = columns // zn
        sums = [
            to(r.inc_out.at[k], r.inc_in.at[k], r.is_send.at[k], r.is_recv.at[k], mem=zpeer[k]) for k in range(1, zn)
        ]
        for k in range(1, zn):
            at = pl.ds(pl.multiple_of(zpeer[k] * strip, strip), strip)
            r.inc_out[k] = r.inc_part[:, at].astype(BF16)
            sums[k - 1].start()
        run = r.inc_part[:, pl.ds(pl.multiple_of(z * strip, strip), strip)]
        for k in range(1, zn):
            sums[k - 1].wait_recv()
            run = run + r.inc_in[k].astype(F32)
        r.inc_all[z] = run.astype(BF16)

        def held(k, a):
            return to(r.inc_all.at[a], r.inc_all.at[a], r.if_send.at[k], r.if_recv.at[a], mem=zpeer[k])

        shares = [held(k, z) for k in range(1, zn)]
        for copy in shares:
            copy.start()
        for k in range(1, zn):
            held(k, zpeer[k]).wait_recv()
        for b in range(zn):
            at = (pl.ds(0, levels), pl.ds(b * strip, strip))
            leaving.append(pltpu.make_async_copy(r.inc_all.at[b], inc_out.at[at], r.out_sem.at[groups + b]))
            leaving[-1].start()
        for copy in sums + shares:
            copy.wait_send()

    with jax.named_scope("drain"):
        for ex in coef_ex + grad_ex:
            ex.drain()
        for gather in gathers:
            gather.drain()
        to(r.pair_out, r.pair_in, r.pair_send, r.pair_recv.at[0], state=partner).wait_send()
        for copy in leaving:
            copy.wait()
        gone = r.rs_out.at[pl.ds(0, (qn - 1) * groups)]
        to(gone, gone, r.rs_send, r.rs_recv.at[0], state=partner).wait_send()


def widen(inc, grad, inc_out, grad_out, inc_in, grad_in, inc_wide, grad_wide, arrive, leave):
    jobs = []
    for k, (src, held, wide, dst) in enumerate([(grad, grad_in, grad_wide, grad_out), (inc, inc_in, inc_wide, inc_out)]):
        half = src.shape[0] // 2
        for h in range(2):
            at, n = pl.ds(h * half, half), 2 * k + h
            jobs.append((
                pltpu.make_async_copy(src.at[at], held.at[at], arrive.at[n]), held.at[at], wide.at[at],
                pltpu.make_async_copy(wide.at[at], dst.at[at], leave.at[n]),
            ))
    for come, _, _, _ in jobs:
        come.start()
    for come, held, wide, go in jobs:
        come.wait()
        wide[...] = held[...].astype(F32)
        go.start()
    for _, _, _, go in jobs:
        go.wait()


def on_device(zn, sn, anomalies, alpha, basis, gradient, vertical_root, band_gain, band, order):
    members, levels, columns = anomalies.shape
    modes = alpha.shape[2]
    rows = members * levels
    qn = sn // 2
    slots = zn * members
    gw = min(LANES, modes)
    groups = modes // gw
    lv = levels // HALVES
    parts = HALVES * groups
    arrivals = 2 if qn == 4 else qn - 1
    width = columns // STRIPS
    line = zn == 4
    hbm = pl.BlockSpec(memory_space=pl.ANY)
    dma = pltpu.SemaphoreType.DMA
    lookup = (1, -(-slots // LANES) * LANES)
    scratch = dict(
        anom=pltpu.VMEM((members, levels, columns), BF16),
        base=pltpu.VMEM((sn, modes, columns), BF16),
        weighted=pltpu.VMEM((rows, columns), BF16),
        alpha=pltpu.VMEM((rows, modes), BF16),
        gradient=pltpu.VMEM((levels, columns), BF16),
        vroot=pltpu.VMEM((levels, levels), F32),
        band=pltpu.VMEM((modes,), jnp.int32),
        gain=pltpu.VMEM((1, modes), F32),
        root_t=pltpu.VMEM((2, GROUP, GROUP), BF16),
        inv_v=pltpu.VMEM(lookup, jnp.int32),
        inv_s=pltpu.SMEM(lookup, jnp.int32),
        coef_pack=pltpu.VMEM((parts, members * lv, gw), BF16),
        pick=pltpu.VMEM((parts, sn, members * lv, gw), BF16),
        pair_out=pltpu.VMEM((groups * qn, rows, gw), F32),
        pair_in=pltpu.VMEM((groups * qn, rows, gw), F32),
        mine=pltpu.VMEM((groups * qn, rows, gw), F32),
        rs_out=pltpu.VMEM((groups * qn, rows, gw), BF16),
        rs_in=pltpu.VMEM((groups * arrivals, rows, gw), BF16),
        relay_in=pltpu.VMEM((groups, rows, gw), BF16),
        grad_pack=pltpu.VMEM((groups, rows, gw), BF16),
        got=pltpu.VMEM((groups, rows, gw), BF16),
        acc=pltpu.VMEM((HALVES, members * lv, columns), F32),
        inc_part=pltpu.VMEM((levels, columns), F32),
        load_sem=dma((7,)),
        out_sem=dma((groups + max(zn, HALVES * STRIPS),)),
        band_gain=pltpu.SMEM(band_gain.shape, F32),
        order=pltpu.SMEM(order.shape, jnp.int32),
        base_sem=dma((groups * qn,)),
        inv_sem=dma,
        z_send=dma((parts,)),
        z_recv=dma((parts,)),
        g_send=dma((groups,)),
        g_recv=dma((groups,)),
        g_rim=dma((groups,)),
        pk_send=dma((parts,)),
        pk_side=dma((parts,)),
        pk_mate=dma((parts,)),
        pk_over=dma((parts,)),
        pk_far=dma((parts,)),
        pk_last=dma((parts,)),
        pair_send=dma,
        pair_recv=dma((groups * qn,)),
        rs_send=dma,
        rs_recv=dma((groups,)),
        relay_recv=dma((groups,)),
    )
    scratch |= {f"coef_held{p}": pltpu.VMEM((slots, lv, gw), BF16) for p in range(parts)}
    scratch |= {f"grad_held{g}": pltpu.VMEM((slots, levels, gw), BF16) for g in range(groups)}
    if line:
        strips = (HALVES, STRIPS, lv, width)
        scratch |= {n: pltpu.VMEM(strips, BF16) for n in ("inc_out", "inc_in", "inc_sum", "inc_got", "inc_all")}
        scratch |= {"inc_send": dma((2,))} | {n: dma((HALVES, STRIPS)) for n in ("inc_recv", "cross_recv")}
    else:
        strips = (zn, levels, columns // zn)
        scratch |= {n: pltpu.VMEM(strips, BF16) for n in ("inc_out", "inc_in", "inc_all")}
        scratch |= {n: dma((zn,)) for n in ("is_send", "is_recv", "if_send", "if_recv")}
    increment, grads = pl.pallas_call(
        functools.partial(kernel, zn, sn, tuple(scratch)),
        out_shape=(
            jax.ShapeDtypeStruct((levels, columns), BF16),
            jax.ShapeDtypeStruct((rows, modes), BF16),
        ),
        in_specs=[hbm] * 8,
        out_specs=(hbm, hbm),
        scratch_shapes=list(scratch.values()),
        compiler_params=pltpu.CompilerParams(
            collective_id=0, has_side_effects=True, vmem_limit_bytes=58 * 2**20
        ),
    )(
        order, band_gain, vertical_root, alpha.reshape(rows, modes), band, gradient,
        anomalies, basis.reshape(sn, modes, columns),
    )
    increment, grads = pl.pallas_call(
        widen,
        out_shape=(
            jax.ShapeDtypeStruct((levels, columns), F32),
            jax.ShapeDtypeStruct((rows, modes), F32),
        ),
        in_specs=[hbm] * 2,
        out_specs=(hbm, hbm),
        scratch_shapes=[
            pltpu.VMEM((levels, columns), BF16),
            pltpu.VMEM((rows, modes), BF16),
            pltpu.VMEM((levels, columns), F32),
            pltpu.VMEM((rows, modes), F32),
            dma((4,)),
            dma((4,)),
        ],
    )(increment, grads)
    return increment, grads.reshape(members, levels, modes)


def solution(mesh):
    zn, sn = mesh.shape["mem"], mesh.shape["state"]
    return jax.shard_map(
        functools.partial(on_device, zn, sn),
        mesh=mesh,
        in_specs=(
            P("mem", None, "state"),
            P("mem", None, "state"),
            P(None, "state"),
            P(None, "state"),
            P(),
            P(),
            P("state"),
            P(),
        ),
        out_specs=(P(None, "state"), P("mem", None, "state")),
        check_vma=False,
    )
```
